32 devices in a mesh: cuts: 4 (over z), tile: 8 (over y, x, core).
Axes of the slice: x: 2, y: 2, z: 4, core: 2. Of those that a mesh axis runs over, the one named last changes fastest.
Arguments:
- probe_wave: float32 [2, 256, 256], replicated, may hold values from -6 to 6
- transmission: float32 [4, 2, 4096, 2048], P('cuts', None, None, 'tile'), may hold values from -1 to 1, as said below
- kernel_phase: float32 [256, 256], replicated, may hold values from -3.140625 to 3.140625
- measured: bfloat16 [8, 6, 256, 256], P('tile'), may hold values from 0 to 4
- counts: int32 [8], P('tile'), may hold values from 1 to 6, as said below
- positions: int32 [8, 6, 2], P('tile'), may hold values from 0 to 3840, as said below
- widths: int32 [8, 2], P('tile'), may hold values from 32 to 128
Outputs:
- adjoint_wave: float32 [4, 8, 6, 2, 256, 256], P('cuts', 'tile')
- object_grad: float32 [4, 2, 4096, 2048], P('cuts', None, None, 'tile')
The draws below stay inside these ranges and needn't reach their ends.
Inputs may be any that keep to these rules, and one draw needn't show every extreme that they name: Every entry has magnitude at most 1; each pair is a complex transmission. Tile t uses its first counts[t] slots; some tile uses all 6 slots. `positions`: rows lie in 0 to 3840 and columns in 0 to 256; column 0 of a tile's extended patch is 128 columns left of its first own column.
All inputs are finite; a program needn't handle non-finite values.
Results may differ from the reference program's by a relative error of at most 0.0003.
Values sent between devices are 32-bit elements; how exact they have to be, the bound alone decides.
A program may use at most 256 MiB of HBM per device.

```python
import math
import jax
import jax.numpy as jnp
from jax import lax

W = 256
TH = 4096
TW = 256
RIM = 128
CAP = 6
SLICES = 1
GROUPS = 4
TILES = 8
NCOL = 2048
NSLICE = 4


def draw_transmission(key, part):
    key_amp, key_phase = jax.random.split(key, 2)
    shape_here = (NSLICE, TH, NCOL)
    amplitude = jax.random.uniform(key_amp, shape_here, jnp.float32, 0.85, 1.0)
    phases = jnp.clip(0.6 * jax.random.normal(key_phase, shape_here, jnp.float32), -1.5, 1.5)
    return jnp.stack([amplitude * jnp.cos(phases), amplitude * jnp.sin(phases)], axis=1)


def draw_counts(key, part):
    key_light = jax.random.fold_in(key, 11)
    key_heavy = jax.random.fold_in(key, 12)
    key_pick = jax.random.fold_in(key, 13)
    light_load = jax.random.randint(key_light, (TILES,), 1, 4)
    heavy_load = jax.random.randint(key_heavy, (TILES,), 0, 4) == 0
    chosen = jax.random.randint(key_pick, (), 0, TILES)
    filled = heavy_load | (jnp.arange(TILES, dtype=jnp.int32) == chosen)
    return jnp.where(filled, CAP, light_load).astype(jnp.int32)


def draw_positions(key, part):
    key_rows = jax.random.fold_in(key, 21)
    key_cols = jax.random.fold_in(key, 22)
    row_place = jax.random.randint(key_rows, (TILES, CAP), 0, TH - W + 1)
    col_place = jax.random.randint(key_cols, (TILES, CAP), 0, TW + 2 * RIM - W + 1)
    return jnp.stack([row_place, col_place], axis=-1).astype(jnp.int32)


def set_ends(values, stream_key, smallest, top_value):
    dims = values.shape
    place = [jax.random.randint(jax.random.fold_in(stream_key, axis), (), 0, dims[axis]) for axis in range(len(dims))]
    values = values.at[tuple(place)].set(smallest)
    longest = dims.index(max(dims))
    place[longest] = (place[longest] + 1) % dims[longest]
    return values.at[tuple(place)].set(top_value)


def shard_levels(stream_key, dims, cuts, smallest, high):
    def one(axis_at, blocks):
        steps = jax.random.uniform(jax.random.fold_in(jax.random.fold_in(stream_key, 6), axis_at), (blocks,), jnp.float32, smallest / len(cuts), high / len(cuts))
        return jnp.repeat(jnp.exp(steps), dims[axis_at] // blocks).reshape((-1,) + (1,) * (len(dims) - axis_at - 1))

    level = one(*cuts[0])
    for cut in cuts[1:]:
        level = level * one(*cut)
    return level


def normal_values(rng, dims, width, reach, kind=jnp.bfloat16):
    values = width * jax.random.normal(rng, dims, jnp.float32)
    return jnp.clip(values, min=-reach, max=reach).astype(kind)


def setup_inputs(seed: int = 0) -> dict:
    key_of = jax.random.split(jax.random.key(seed), 8)
    return {
        "probe_wave": normal_values(key_of[0], (2, W, W), 1.0, 6.0, jnp.float32),
        "transmission": draw_transmission(jax.random.fold_in(key_of[7], 71), 0),
        "kernel_phase": jnp.clip(jax.random.uniform(key_of[2], (W, W), jnp.float32, -3.140625, 3.140625), -3.140625, 3.140625),
        "measured": jnp.clip(4.0 * jax.random.uniform(key_of[3], (TILES, CAP, W, W), jnp.float32) ** shard_levels(key_of[3], (TILES, CAP, W, W), ((0, 8),), -0.2, 0.2), 0.0, 4.0).astype(jnp.bfloat16),
        "counts": draw_counts(jax.random.fold_in(key_of[7], 71), 0),
        "positions": draw_positions(jax.random.fold_in(key_of[7], 71), 0),
        "widths": set_ends(jax.random.randint(key_of[6], (TILES, 2), RIM // 4, RIM + 1), jax.random.fold_in(key_of[6], 1), RIM // 4, RIM).astype(jnp.int32),
    }


def make_tables():
    indices = jnp.arange(W, dtype=jnp.int32)
    product = indices[:, None] * indices[None, :] % W
    angles = product.astype(jnp.float32) * (2.0 * math.pi / W)
    cosine = jnp.cos(angles) / math.sqrt(W)
    sine_part = jnp.sin(angles) / math.sqrt(W)
    forward = jnp.concatenate([jnp.concatenate([cosine, sine_part], 1), jnp.concatenate([-sine_part, cosine], 1)], 0)
    inverse = jnp.concatenate([jnp.concatenate([cosine, -sine_part], 1), jnp.concatenate([sine_part, cosine], 1)], 0)
    return (forward, inverse)

def transform(fields, matrix):
    number = fields.shape[0]
    stacked = fields.reshape(number, 2 * W, W)
    halfway = jnp.einsum('ab,pbc->pac', matrix, stacked, precision=lax.Precision.HIGHEST)
    halfway = halfway.reshape(number, 2, W, W)
    quadrant = matrix.reshape(2, W, 2, W)
    return jnp.einsum('psik,rjsk->prij', halfway, quadrant, precision=lax.Precision.HIGHEST)

def complex_mul(first_op, second_op):
    first_re, first_im = (first_op[..., 0, :, :], first_op[..., 1, :, :])
    second_re, second_im = (second_op[..., 0, :, :], second_op[..., 1, :, :])
    return jnp.stack([first_re * second_re - first_im * second_im, first_re * second_im + first_im * second_re], axis=-3)

def conj_mul(first_op, second_op):
    first_re, first_im = (first_op[..., 0, :, :], first_op[..., 1, :, :])
    second_re, second_im = (second_op[..., 0, :, :], second_op[..., 1, :, :])
    return jnp.stack([first_re * second_re + first_im * second_im, first_re * second_im - first_im * second_re], axis=-3)

def propagate(fields, kernel, tables):
    spectrum = transform(fields, tables[0])
    return transform(complex_mul(kernel, spectrum), tables[1])

def keep_columns(tile_at, width_pair):
    columns = jnp.arange(TW + 2 * RIM, dtype=jnp.int32)
    globally = tile_at * TW - RIM + columns
    inside = (globally >= 0) & (globally < TILES * TW)
    middle = (columns >= RIM) & (columns < RIM + TW)
    left_ok = (columns < RIM) & (RIM - columns <= width_pair[0])
    right_ok = (columns >= RIM + TW) & (columns - RIM - TW + 1 <= width_pair[1])
    return inside & (middle | left_ok | right_ok)

def cut_windows(grad_plane, places):
    anchor = jnp.zeros((), jnp.int32)

    def single(corner):
        return lax.dynamic_slice(grad_plane, (anchor, corner[0], corner[1]), (2, W, W))
    return jax.vmap(single)(places)

def add_windows(grad_plane, places, contrib):
    anchor = jnp.zeros((), jnp.int32)
    for item_at in range(contrib.shape[0]):
        corner_at = (anchor, places[item_at, 0], places[item_at, 1])
        current = lax.dynamic_slice(grad_plane, corner_at, (2, W, W))
        grad_plane = lax.dynamic_update_slice(grad_plane, current + contrib[item_at], corner_at)
    return grad_plane

def reference(probe_wave, transmission, kernel_phase, measured, counts, positions, widths):
    tables = make_tables()
    kernel = jnp.stack([jnp.cos(kernel_phase), jnp.sin(kernel_phase)], 0)
    kernel_conj = jnp.stack([jnp.cos(kernel_phase), -jnp.sin(kernel_phase)], 0)
    padded = jnp.pad(transmission, ((0, 0), (0, 0), (0, 0), (RIM, RIM)))
    vacuum = jnp.array([1.0, 0.0], dtype=jnp.float32)[:, None, None]

    def one_tile(operands):
        tile_at, count_here, places, width_pair, observed = operands
        keep_mask = keep_columns(tile_at, width_pair)
        object_patch = lax.dynamic_slice_in_dim(padded, tile_at * TW, TW + 2 * RIM, 3)
        object_patch = jnp.where(keep_mask, object_patch, vacuum)
        live_slots = (jnp.arange(CAP, dtype=jnp.int32) < count_here).astype(jnp.float32)
        fields = probe_wave[None] * live_slots[:, None, None, None]
        saved_waves = []
        window_list = []
        for slice_at in range(NSLICE):
            windows = cut_windows(object_patch[slice_at], places)
            saved_waves.append(fields)
            window_list.append(windows)
            fields = propagate(complex_mul(windows, fields), kernel, tables)
        far_field = transform(fields, tables[0])
        intensity = far_field[:, 0] * far_field[:, 0] + far_field[:, 1] * far_field[:, 1]
        residual = intensity - observed.astype(jnp.float32)
        backward = transform(far_field * residual[:, None], tables[1])
        grad_list = []
        entry_list = [None] * GROUPS
        for slice_at in reversed(range(NSLICE)):
            turned = propagate(backward, kernel_conj, tables)
            contrib = conj_mul(saved_waves[slice_at], turned)
            grad_plane = add_windows(jnp.zeros_like(object_patch[slice_at]), places, contrib)
            grad_list.insert(0, jnp.where(keep_mask, grad_plane, 0.0))
            backward = conj_mul(window_list[slice_at], turned)
            if slice_at % SLICES == 0:
                entry_list[slice_at // SLICES] = backward
        grad_patch = jnp.stack(grad_list, 0)
        return (jnp.stack(entry_list, 0), grad_patch[..., :RIM], grad_patch[..., RIM:RIM + TW], grad_patch[..., RIM + TW:])
    tile_ids = jnp.arange(TILES, dtype=jnp.int32)
    entries, left_rims, center, right_rims = lax.map(one_tile, (tile_ids, counts, positions, widths, measured))
    from_left = jnp.concatenate([jnp.zeros_like(right_rims[:1]), right_rims[:-1]], 0)
    from_right = jnp.concatenate([left_rims[1:], jnp.zeros_like(left_rims[:1])], 0)
    center = center.at[..., :RIM].add(from_left)
    center = center.at[..., TW - RIM:].add(from_right)
    object_grad = jnp.moveaxis(center, 0, 3).reshape(NSLICE, 2, TH, NCOL)
    adjoint_wave = jnp.swapaxes(entries, 0, 1)
    return (adjoint_wave, object_grad)
```

```python
import functools
import math

import jax
import jax.numpy as jnp
import numpy as np
from jax import lax
from jax.experimental import pallas as pl
from jax.experimental.pallas import tpu as pltpu
from jax.sharding import PartitionSpec as P

RIM = 128
PAD = 8
MESH = pl.DeviceIdType.MESH
VMEM_LIMIT = 60 * 1024 * 1024


def params(**kw):
    return pltpu.CompilerParams(vmem_limit_bytes=VMEM_LIMIT, **kw)


def vmem():
    return pl.BlockSpec(memory_space=pltpu.VMEM)


def smem():
    return pl.BlockSpec(memory_space=pltpu.SMEM)


def shift(value, axis, by):
    count = lax.axis_size(axis)
    pairs = [(i, i + by) for i in range(count) if 0 <= i + by < count]
    return lax.ppermute(value, axis, pairs)


def make_tables(extent):
    half = extent // 2
    indices = np.arange(extent)
    angles = (indices[:, None] * indices[None, :] % extent) * (2.0 * math.pi / extent)
    cosine = (np.cos(angles) / math.sqrt(extent)).astype(np.float32)
    sine = (np.sin(angles) / math.sqrt(extent)).astype(np.float32)
    tables = []
    for parity in range(2):
        c, s = cosine[parity::2, :half], sine[parity::2, :half]
        block = np.block([[c, s], [-s, c]])
        for matrix in (block, block.T):
            hi = matrix.astype(jnp.bfloat16)
            lo = (matrix - hi.astype(np.float32)).astype(jnp.bfloat16)
            tables += [jnp.asarray(hi), jnp.asarray(lo)]
    order = np.concatenate([indices[0::2], indices[1::2]])
    sort = (order[:, None] == indices[None, :]).astype(jnp.bfloat16)
    return tables + [jnp.asarray(sort), jnp.asarray(np.ascontiguousarray(sort.T))]


def aligned(row, limit):
    base = jnp.minimum(row // PAD * PAD, limit)
    return pl.multiple_of(base, PAD), row - base


def extract_kernel(here, left_pos, right_pos, own_pos, trans, own, to_left, to_right,
                   buf_own, buf_left, buf_right, sems):
    slots, _, extent, _ = own.shape
    rows, cols = trans.shape[1:]
    tall = extent + PAD
    slack = cols + 2 * RIM - extent
    jobs = (
        (left_pos, buf_left, 0, RIM),
        (right_pos, buf_right, cols - RIM, RIM),
        (own_pos, buf_own, 0, cols),
    )

    def copy(j, s):
        pos, buf, start, width = jobs[j]
        base, off = aligned(pos[s, 0], rows - tall)
        src = trans.at[:, pl.ds(base, tall), pl.ds(start, width)]
        return pltpu.make_async_copy(src, buf.at[s], sems.at[j, s]), off

    for j in range(3):
        for s in range(slots):
            copy(j, s)[0].start()

    def columns(width):
        return lax.broadcasted_iota(jnp.int32, (extent, width), 1)

    def load(j, s, p, off, turn):
        value = pltpu.roll(jobs[j][1][s, p], (tall - off) % tall, 0)[:extent]
        return pltpu.roll(value, turn, 1)

    def for_left(s, carry):
        one, off = copy(0, s)
        one.wait()
        short = slack - left_pos[s, 1]
        at = columns(RIM) - short
        good = (at >= 0) & (at + 1 <= left_pos[slots, 1])
        for p in range(2):
            value = load(0, s, p, off, short % RIM)
            to_left[s, p] = jnp.where(good, value, 0.0)
        return carry

    def for_right(s, carry):
        one, off = copy(1, s)
        one.wait()
        col = right_pos[s, 1]
        at = columns(RIM) + col
        good = (at < RIM) & (RIM - at <= right_pos[slots, 0])
        for p in range(2):
            value = load(1, s, p, off, (cols - col) % RIM)
            to_right[s, p] = jnp.where(good, value, 0.0)
        return carry

    def for_own(s, carry):
        one, off = copy(2, s)
        one.wait()
        col = own_pos[s, 1]
        at = columns(extent) + col
        middle = (at >= RIM) & (at < RIM + cols)
        left_ok = (here[0] > 0) & (at < RIM) & (RIM - at <= own_pos[slots, 0])
        right_ok = (here[0] < here[1] - 1) & (at >= RIM + cols) & (
            at - RIM - cols + 1 <= own_pos[slots, 1])
        rim = left_ok | right_ok
        for p in range(2):
            value = load(2, s, p, off, (cols + RIM - col) % cols)
            out = jnp.where(rim, 0.0, 1.0 - p)
            own[s, p] = jnp.where(middle, value, out)
        return carry

    lax.fori_loop(0, slots, for_left, 0)
    lax.fori_loop(0, slots, for_right, 0)
    lax.fori_loop(0, slots, for_own, 0)


def gather_kernel(left_pos, right_pos, own_pos, contrib, from_left, from_right, out):
    slots, _, extent, _ = contrib.shape
    rows, cols = out.shape[1:]
    tall = extent + PAD
    slack = cols + 2 * RIM - extent
    out[...] = jnp.zeros(out.shape, out.dtype)

    def columns(width):
        return lax.broadcasted_iota(jnp.int32, (extent, width), 1)

    def add(source, s, pos, good, turn, start, width):
        base, off = aligned(pos[s, 0], rows - tall)
        for p in range(2):
            value = jnp.where(good, pltpu.roll(source[s, p], turn, 1), 0.0)
            value = jnp.concatenate([value, jnp.zeros((PAD, width), jnp.float32)], axis=0)
            value = pltpu.roll(value, off, 0)
            out[p, pl.ds(base, tall), pl.ds(start, width)] += value

    def body(s, carry):
        col = own_pos[s, 1]
        at = columns(cols) + RIM - col
        good = (at >= 0) & (at < extent)
        add(contrib, s, own_pos, good, (col + cols - RIM) % cols, 0, cols)
        short = slack - left_pos[s, 1]
        at = columns(RIM)
        good = (at + short < RIM) & (at + 1 <= left_pos[slots, 1])
        add(from_left, s, left_pos, good, (cols - short) % RIM, 0, RIM)
        col = right_pos[s, 1]
        good = (at >= col) & (RIM - at <= right_pos[slots, 0])
        add(from_right, s, right_pos, good, col % RIM, cols - RIM, RIM)
        return carry

    lax.fori_loop(0, slots, body, 0)


def pipeline_kernel(sections, tiles, live, to_left, to_right, own, probe, phase_kernel, measured,
                    ef_hi, ef_lo, ei_hi, ei_lo, of_hi, of_lo, oi_hi, oi_lo, sort, unsort, adjoint, contrib, from_left, from_right,
                    windows, left_rim, right_rim, got_left, got_right,
                    arrived, leaving, backed, ahead, lefts, rights, turn,
                    talls, wides, freq, spectrum, send_f, recv_f, send_b, recv_b,
                    send_w, recv_w, send_rim, recv_rim, send_got, recv_got, token):
    g = lax.axis_index("cuts")
    t = lax.axis_index("tile")
    last = sections - 1
    mid = last - 1
    end = tiles - 1
    slots, _, extent, _ = own.shape
    h = extent // 2
    partner = t + 1 - 2 * (t % 2)

    barrier = pltpu.get_barrier_semaphore()

    @pl.when(g > 0)
    def _():
        pl.semaphore_signal(barrier, inc=1, device_id={"cuts": g - 1}, device_id_type=MESH)

    @pl.when(g < last)
    def _():
        pl.semaphore_signal(barrier, inc=1, device_id={"cuts": g + 1}, device_id_type=MESH)

    @pl.when(t > 0)
    def _():
        pl.semaphore_signal(barrier, inc=1, device_id={"tile": t - 1}, device_id_type=MESH)

    @pl.when(t < end)
    def _():
        pl.semaphore_signal(barrier, inc=1, device_id={"tile": t + 1}, device_id_type=MESH)

    peers = (g + last - 1) // last + 1 - g // last + (t + end - 1) // end + 1 - t // end
    pl.semaphore_wait(barrier, peers)

    def rim_copy(side, s):
        src, dst = ((to_left, right_rim), (to_right, left_rim))[side]
        return pltpu.make_async_remote_copy(
            src_ref=src.at[s], dst_ref=dst.at[s], send_sem=send_rim.at[side, s],
            recv_sem=recv_rim.at[side, s], device_id={"tile": t + (-1, 1)[side]},
            device_id_type=MESH)

    def got_copy(side, s):
        start, dst = ((0, got_right), (extent - RIM, got_left))[side]
        return pltpu.make_async_remote_copy(
            src_ref=contrib.at[s, :, :, pl.ds(start, RIM)], dst_ref=dst.at[s],
            send_sem=send_got.at[side, s], recv_sem=recv_got.at[side, s],
            device_id={"tile": t + (-1, 1)[side]}, device_id_type=MESH)

    def each(action):
        def body(s, carry):
            action(s)
            return carry

        lax.fori_loop(0, slots, body, 0)

    @pl.when(t > 0)
    def _():
        each(lambda s: rim_copy(0, s).start())

    @pl.when(t < end)
    def _():
        each(lambda s: rim_copy(1, s).start())

    @pl.when(t == 0)
    def _():
        left_rim[...] = jnp.zeros(left_rim.shape, left_rim.dtype)
        got_left[...] = jnp.zeros(got_left.shape, got_left.dtype)

    @pl.when(t == end)
    def _():
        right_rim[...] = jnp.zeros(right_rim.shape, right_rim.dtype)
        got_right[...] = jnp.zeros(got_right.shape, got_right.dtype)

    forms = ((ef_hi, ef_lo, ei_hi, ei_lo), (of_hi, of_lo, oi_hi, oi_lo))
    for parity in range(2):
        fh, fl, ih, il = forms[parity]
        for inverse, (lh, ll, rh, rl) in enumerate(((fh, fl, ih, il), (ih, il, fh, fl))):
            at = 2 * inverse + parity
            lefts[at, :, :extent] = lh[...]
            lefts[at, :, extent : 2 * extent] = lh[...]
            lefts[at, :, 2 * extent :] = ll[...]
            rights[at, :extent] = rh[...]
            rights[at, extent : 2 * extent] = rh[...]
            rights[at, 2 * extent :] = rl[...]

    def exact(x, y):
        return jnp.dot(x, y, preferred_element_type=jnp.float32)

    for p in range(2):
        rest = phase_kernel[p]
        total = jnp.zeros((extent, extent), jnp.float32)
        for _ in range(3):
            part = rest.astype(jnp.bfloat16)
            rest = rest - part.astype(jnp.float32)
            rows = exact(sort[...], part).astype(jnp.bfloat16)
            total += exact(rows, unsort[...])
        turn[p] = total
    turn[2] = -turn[1]

    def split(value):
        hi = value.astype(jnp.bfloat16)
        lo = (value - hi.astype(jnp.float32)).astype(jnp.bfloat16)
        return (hi, lo, hi)

    def put_tall(parity, p, value):
        for at, part in enumerate(split(value)):
            talls[parity, pl.ds(at * extent + p * h, h), :] = part

    def put_wide(parity, rows, p, value):
        n = value.shape[0]
        for at, part in enumerate(split(value)):
            wides[parity, pl.ds(rows, n), pl.ds(at * extent + p * h, h)] = part

    def left(at):
        return exact(lefts[at], talls[at % 2])

    def right(at):
        return exact(wides[at % 2], rights[at])

    def to_freq():
        for p in range(2):
            put_tall(0, p, spectrum[p, :h] + spectrum[p, h:])
            put_tall(1, p, spectrum[p, :h] - spectrum[p, h:])
        for block in range(2):
            half = left(block)
            for p in range(2):
                value = half[p * h : (p + 1) * h]
                put_wide(0, block * h, p, value[:, :h] + value[:, h:])
                put_wide(1, block * h, p, value[:, :h] - value[:, h:])
        for parity in range(2):
            freq[parity] = right(parity)

    def from_freq():
        u, v = right(2), right(3)
        for p in range(2):
            up, vp = u[:, p * h : (p + 1) * h], v[:, p * h : (p + 1) * h]
            plus, minus = up + vp, up - vp
            for parity in range(2):
                rows = slice(parity * h, (parity + 1) * h)
                both = jnp.concatenate([plus[rows], minus[rows]], axis=1)
                put_tall(parity, p, both)
        u, v = left(2), left(3)
        for p in range(2):
            up, vp = u[p * h : (p + 1) * h], v[p * h : (p + 1) * h]
            spectrum[p, :h] = up + vp
            spectrum[p, h:] = up - vp

    def send_forward(s, part):
        return pltpu.make_async_remote_copy(
            src_ref=leaving.at[s, part], dst_ref=arrived.at[s, part], send_sem=send_f.at[s, part],
            recv_sem=recv_f.at[s, part], device_id={"cuts": g + 1}, device_id_type=MESH)

    def send_backward(s):
        return pltpu.make_async_remote_copy(
            src_ref=adjoint.at[s], dst_ref=backed.at[s], send_sem=send_b.at[s],
            recv_sem=recv_b.at[s], device_id={"cuts": g - 1}, device_id_type=MESH)

    def send_window(s):
        return pltpu.make_async_remote_copy(
            src_ref=windows.at[s], dst_ref=ahead.at[s], send_sem=send_w.at[s],
            recv_sem=recv_w.at[s], device_id={"cuts": g - 1}, device_id_type=MESH)

    def compose(s):
        @pl.when(t < end)
        def _():
            rim_copy(0, s).wait_recv()

        @pl.when(t > 0)
        def _():
            rim_copy(1, s).wait_recv()

        for p in range(2):
            windows[s, p, :, :RIM] = own[s, p, :, :RIM] + left_rim[s, p]
            if extent > 2 * RIM:
                windows[s, p, :, RIM : extent - RIM] = own[s, p, :, RIM : extent - RIM]
            windows[s, p, :, extent - RIM :] = own[s, p, :, extent - RIM :] + right_rim[s, p]

    def product(w, x, s, sign):
        wr, wi = w[s, 0], w[s, 1]
        xr, xi = x
        spectrum[0] = wr * xr - sign * (wi * xi)
        spectrum[1] = wr * xi + sign * (wi * xr)

    @pl.when(g == last)
    def _():
        def body(s):
            compose(s)
            send_window(s).start()

        each(body)

    def event(s, op):
        @pl.when(op == 0)
        def _():
            @pl.when(g == 0)
            def _():
                arrived[s] = probe[...] * live[s]

            @pl.when(g > 0)
            def _():
                send_forward(s, 0).wait_recv()
                send_forward(s, 1).wait_recv()

            @pl.when(g < last)
            def _():
                compose(s)

            product(windows, (arrived[s, 0], arrived[s, 1]), s, 1.0)

        @pl.when(op == 1)
        def _():
            send_window(s).wait_recv()
            product(ahead, (spectrum[0], spectrum[1]), s, 1.0)

        @pl.when((op == 4) & (g < mid))
        def _():
            send_backward(s).wait_recv()
            spectrum[...] = backed[s]

        @pl.when((op == 4) & (g == mid))
        def _():
            product(ahead, (spectrum[0], spectrum[1]), s, -1.0)

        to_freq()

        @pl.when(op == 2)
        def _():
            seen = exact(sort[...], measured[s]).astype(jnp.bfloat16)
            seen = exact(seen, unsort[...])
            for parity in range(2):
                fr, fi = freq[parity, :, :h], freq[parity, :, h:]
                residual = fr * fr + fi * fi - seen[:, parity * h : (parity + 1) * h]
                put_wide(parity, 0, 0, fr * residual)
                put_wide(parity, 0, 1, fi * residual)

        @pl.when(op != 2)
        def _():
            sine = 1 + op // 3
            for parity in range(2):
                cols = slice(parity * h, (parity + 1) * h)
                kr, ki = turn[0, :, cols], turn[sine, :, cols]
                xr, xi = freq[parity, :, :h], freq[parity, :, h:]
                put_wide(parity, 0, 0, kr * xr - ki * xi)
                put_wide(parity, 0, 1, kr * xi + ki * xr)

        from_freq()

        @pl.when((op == 0) & (g < last))
        def _():
            leaving[s] = spectrum[...]

            @pl.when((g == 0) & ((s > 0) | (t % 2 == 1)))
            def _():
                pl.semaphore_wait(token, 1)

            send_forward(s, 0).start()
            send_forward(s, 1).start()

            @pl.when(g == 0)
            def _():
                send_forward(s, 0).wait_send()

                @pl.when((s < slots - 1) | (t % 2 == 0))
                def _():
                    pl.semaphore_signal(token, inc=1, device_id={"tile": partner}, device_id_type=MESH)

        @pl.when(((op == 3) & (g == last)) | (op == 4))
        def _():
            tr, ti = spectrum[0], spectrum[1]
            wr, wi = windows[s, 0], windows[s, 1]
            adjoint[s, 0] = wr * tr + wi * ti
            adjoint[s, 1] = wr * ti - wi * tr

            @pl.when((g > 0) & (g < last))
            def _():
                send_backward(s).start()

            xr, xi = arrived[s, 0], arrived[s, 1]
            contrib[s, 0] = xr * tr + xi * ti
            contrib[s, 1] = xr * ti - xi * tr

            @pl.when(t > 0)
            def _():
                got_copy(0, s).start()

            @pl.when(t < end)
            def _():
                got_copy(1, s).start()

    lag = 2 * (mid - g)
    early = (g < mid).astype(jnp.int32)
    final = g // last
    ops = 5 - 3 * early - 2 * final
    count = (slots + early * lag) * ops

    def step(e, carry):
        k, part = e // ops, e % ops
        s = k - early * part * lag
        op = part + early * part * 3 + final * ((part + 1) // 2)

        @pl.when((s >= 0) & (s < slots))
        def _():
            event(s, op)

        return carry

    lax.fori_loop(0, count, step, 0)

    @pl.when(g < last)
    def _():
        each(lambda s: send_forward(s, 1).wait_send())

    @pl.when((g > 0) & (g < last))
    def _():
        each(lambda s: send_forward(s, 0).wait_send())
        each(lambda s: send_backward(s).wait_send())

    @pl.when(g == last)
    def _():
        each(lambda s: send_window(s).wait_send())

    @pl.when(t < end)
    def _():
        each(lambda s: got_copy(0, s).wait_recv())

    @pl.when(t > 0)
    def _():
        each(lambda s: got_copy(1, s).wait_recv())

    def finish(side):
        def body(s):
            rim_copy(side, s).wait_send()
            got_copy(side, s).wait_send()

        each(body)

    @pl.when(t > 0)
    def _():
        finish(0)

    @pl.when(t < end)
    def _():
        finish(1)

    from_left[...] = got_left[...]
    from_right[...] = got_right[...]


def on_device(probe_wave, transmission, kernel_phase, measured, counts, positions, widths):
    f32 = jnp.float32
    rows, cols = transmission.shape[2:]
    extent = probe_wave.shape[-1]
    slots = positions.shape[1]
    sections = lax.axis_size("cuts")
    tiles_total = lax.axis_size("tile")
    tile_at = lax.axis_index("tile")
    tall = extent + PAD
    trans = transmission[0]
    own_pos = jnp.concatenate([positions[0], widths], 0)
    right_pos = shift(own_pos, "tile", -1)
    left_pos = shift(own_pos, "tile", 1)
    here = jnp.stack([tile_at, jnp.asarray(tiles_total, tile_at.dtype)]).astype(jnp.int32)
    sds = jax.ShapeDtypeStruct
    wave = sds((slots, 2, extent, extent), f32)
    rim = sds((slots, 2, extent, RIM), f32)
    assert extent == cols and extent >= 2 * RIM

    own, to_left, to_right = pl.pallas_call(
        extract_kernel,
        out_shape=(wave, rim, rim),
        in_specs=[smem()] * 4 + [pl.BlockSpec(memory_space=pl.ANY)],
        out_specs=(vmem(), vmem(), vmem()),
        scratch_shapes=[
            pltpu.VMEM((slots, 2, tall, cols), f32),
            pltpu.VMEM((slots, 2, tall, RIM), f32),
            pltpu.VMEM((slots, 2, tall, RIM), f32),
            pltpu.SemaphoreType.DMA((3, slots)),
        ],
        compiler_params=params(),
    )(here, left_pos, right_pos, own_pos, trans)

    tables = make_tables(extent)
    phase_kernel = jnp.stack([jnp.cos(kernel_phase), jnp.sin(kernel_phase)], 0)
    live = (jnp.arange(slots, dtype=jnp.int32) < counts[0]).astype(f32)
    waves = pltpu.VMEM((slots, 2, extent, extent), f32)
    bf16 = jnp.bfloat16
    rims = pltpu.VMEM((slots, 2, extent, RIM), f32)
    adjoint, contrib, from_left, from_right = pl.pallas_call(
        functools.partial(pipeline_kernel, sections, tiles_total),
        out_shape=(wave, wave, rim, rim),
        in_specs=[smem()] + [vmem()] * 16,
        out_specs=(vmem(),) * 4,
        scratch_shapes=[
            waves, rims, rims, rims, rims,
            waves, waves, waves, waves,
            pltpu.VMEM((4, extent, 3 * extent), bf16),
            pltpu.VMEM((4, 3 * extent, extent), bf16),
            pltpu.VMEM((3, extent, extent), f32),
            pltpu.VMEM((2, 3 * extent, extent), bf16),
            pltpu.VMEM((2, extent, 3 * extent), bf16),
            pltpu.VMEM((2, extent, extent), f32),
            pltpu.VMEM((2, extent, extent), f32),
            pltpu.SemaphoreType.DMA((slots, 2)),
            pltpu.SemaphoreType.DMA((slots, 2)),
            pltpu.SemaphoreType.DMA((slots,)),
            pltpu.SemaphoreType.DMA((slots,)),
            pltpu.SemaphoreType.DMA((slots,)),
            pltpu.SemaphoreType.DMA((slots,)),
            pltpu.SemaphoreType.DMA((2, slots)),
            pltpu.SemaphoreType.DMA((2, slots)),
            pltpu.SemaphoreType.DMA((2, slots)),
            pltpu.SemaphoreType.DMA((2, slots)),
            pltpu.SemaphoreType.REGULAR,
        ],
        compiler_params=params(collective_id=0, has_side_effects=True),
    )(live, to_left, to_right, own, probe_wave, phase_kernel, measured[0], *tables)

    grad = pl.pallas_call(
        gather_kernel,
        out_shape=sds((2, rows, cols), f32),
        in_specs=[smem()] * 3 + [vmem()] * 3,
        out_specs=vmem(),
        compiler_params=params(),
    )(left_pos, right_pos, own_pos, contrib, from_left, from_right)
    return (adjoint[None, None], grad[None])


def solution(mesh):
    return jax.shard_map(
        on_device,
        mesh=mesh,
        in_specs=(
            P(),
            P("cuts", None, None, "tile"),
            P(),
            P("tile", None, None, None),
            P("tile"),
            P("tile", None, None),
            P("tile", None),
        ),
        out_specs=(P("cuts", "tile", None, None, None, None), P("cuts", None, None, "tile")),
        check_vma=False,
    )
```

```python
import functools
import math

import jax
import jax.numpy as jnp
import numpy as np
from jax import lax
from jax.experimental import pallas as pl
from jax.experimental.pallas import tpu as pltpu
from jax.sharding import PartitionSpec as P

RIM = 128
PAD = 8
MESH = pl.DeviceIdType.MESH
MIB = 1024 * 1024
EXTRACT_VMEM = 62 * MIB
PIPELINE_VMEM = 62 * MIB
GATHER_VMEM = 62 * MIB


def params(limit, **kw):
    return pltpu.CompilerParams(vmem_limit_bytes=limit, **kw)


def vmem():
    return pl.BlockSpec(memory_space=pltpu.VMEM)


def smem():
    return pl.BlockSpec(memory_space=pltpu.SMEM)


def shift(value, axis, by):
    count = lax.axis_size(axis)
    pairs = [(i, i + by) for i in range(count) if 0 <= i + by < count]
    return lax.ppermute(value, axis, pairs)


def make_tables(extent):
    half = extent // 2
    indices = np.arange(extent)
    angles = (indices[:, None] * indices[None, :] % extent) * (2.0 * math.pi / extent)
    cosine = (np.cos(angles) / math.sqrt(extent)).astype(np.float32)
    sine = (np.sin(angles) / math.sqrt(extent)).astype(np.float32)
    tables = []
    for parity in range(2):
        c, s = cosine[parity::2, :half], sine[parity::2, :half]
        block = np.block([[c, s], [-s, c]])
        for matrix in (block, block.T):
            hi = matrix.astype(jnp.bfloat16)
            lo = (matrix - hi.astype(np.float32)).astype(jnp.bfloat16)
            tables += [jnp.asarray(hi), jnp.asarray(lo)]
    order = np.concatenate([indices[0::2], indices[1::2]])
    sort = (order[:, None] == indices[None, :]).astype(jnp.bfloat16)
    return tables + [jnp.asarray(sort), jnp.asarray(np.ascontiguousarray(sort.T))]


def aligned(row, limit):
    base = jnp.minimum(row // PAD * PAD, limit)
    return pl.multiple_of(base, PAD), row - base


def extract_kernel(left_pos, right_pos, own_pos, trans, own, to_left, to_right,
                   buf_left, buf_right, buf_own, out_left, out_right, out_own, sem_in, sem_out):
    t = lax.axis_index("tile")
    end = lax.axis_size("tile") - 1
    slots, _, extent, _ = own.shape
    rows, cols = trans.shape[1:]
    tall = extent + PAD
    slack = cols + 2 * RIM - extent
    jobs = (
        (left_pos, buf_left, 0, RIM, out_left, to_left),
        (right_pos, buf_right, cols - RIM, RIM, out_right, to_right),
        (own_pos, buf_own, 0, cols, out_own, own),
    )

    def fetch(j, s):
        pos, buf, start, width = jobs[j][:4]
        base, off = aligned(pos[0, s], rows - tall)
        src = trans.at[:, pl.ds(base, tall), pl.ds(start, width)]
        return pltpu.make_async_copy(src, buf.at[s], sem_in.at[j, s]), off

    def flush(j, s):
        return pltpu.make_async_copy(jobs[j][4].at[s], jobs[j][5].at[s], sem_out.at[j, s])

    for s in range(slots):
        for j in range(3):
            fetch(j, s)[0].start()

    def columns(width):
        return lax.broadcasted_iota(jnp.int32, (extent, width), 1)

    def load(j, s, p, off, turn):
        value = pltpu.roll(jobs[j][1][s, p], (tall - off) % tall, 0)[:extent]
        return pltpu.roll(value, turn, 1)

    def body(s, carry):
        one, off = fetch(0, s)
        one.wait()
        short = slack - left_pos[1, s]
        at = columns(RIM) - short
        good = (at >= 0) & (at + 1 <= left_pos[1, slots])
        for p in range(2):
            out_left[s, p] = jnp.where(good, load(0, s, p, off, short % RIM), 0.0)
        flush(0, s).start()
        one, off = fetch(1, s)
        one.wait()
        col = right_pos[1, s]
        at = columns(RIM) + col
        good = (at < RIM) & (RIM - at <= right_pos[0, slots])
        for p in range(2):
            out_right[s, p] = jnp.where(good, load(1, s, p, off, (cols - col) % RIM), 0.0)
        flush(1, s).start()
        one, off = fetch(2, s)
        one.wait()
        col = own_pos[1, s]
        at = columns(extent) + col
        middle = (at >= RIM) & (at < RIM + cols)
        left_ok = (t > 0) & (at < RIM) & (RIM - at <= own_pos[0, slots])
        right_ok = (t < end) & (at >= RIM + cols) & (at - RIM - cols + 1 <= own_pos[1, slots])
        rim = left_ok | right_ok
        for p in range(2):
            value = load(2, s, p, off, (cols + RIM - col) % cols)
            out_own[s, p] = jnp.where(middle, value, jnp.where(rim, 0.0, 1.0 - p))
        flush(2, s).start()
        return carry

    lax.fori_loop(0, slots, body, 0)
    for s in range(slots):
        for j in range(3):
            flush(j, s).wait()


def gather_kernel(left_pos, right_pos, own_pos, contrib, from_left,
                  from_right, adjoint, grad, entry, acc, buf_own, buf_left, buf_right, buf_entry,
                  sem_in, sem_entry, sem_grad):
    slots, _, extent, _ = buf_own.shape
    rows, cols = acc.shape[1:]
    tall = extent + PAD
    slack = cols + 2 * RIM - extent
    jobs = ((contrib, buf_own), (from_left, buf_left), (from_right, buf_right))

    def fetch(j, s):
        return pltpu.make_async_copy(jobs[j][0].at[s], jobs[j][1].at[s], sem_in.at[j, s])

    for s in range(slots):
        for j in range(3):
            fetch(j, s).start()
    entry_in = pltpu.make_async_copy(adjoint, buf_entry, sem_entry.at[0])
    entry_out = pltpu.make_async_copy(buf_entry, entry, sem_entry.at[1])
    entry_in.start()
    acc[...] = jnp.zeros(acc.shape, acc.dtype)

    def columns(width):
        return lax.broadcasted_iota(jnp.int32, (extent, width), 1)

    def add(source, s, p, row, good, turn, start, width):
        base, off = aligned(row, rows - tall)
        value = jnp.where(good, pltpu.roll(source[s, p], turn, 1), 0.0)
        value = jnp.concatenate([value, jnp.zeros((PAD, width), jnp.float32)], axis=0)
        acc[p, pl.ds(base, tall), pl.ds(start, width)] += pltpu.roll(value, off, 0)

    def plane(p):
        def body(s, carry):
            if p == 0:
                for j in range(3):
                    fetch(j, s).wait()
            col = own_pos[1, s]
            at = columns(cols) + RIM - col
            good = (at >= 0) & (at < extent)
            add(buf_own, s, p, own_pos[0, s], good, (col + cols - RIM) % cols, 0, cols)
            short = slack - left_pos[1, s]
            at = columns(RIM)
            good = (at + short < RIM) & (at + 1 <= left_pos[1, slots])
            add(buf_left, s, p, left_pos[0, s], good, (cols - short) % RIM, 0, RIM)
            col = right_pos[1, s]
            good = (at >= col) & (RIM - at <= right_pos[0, slots])
            add(buf_right, s, p, right_pos[0, s], good, col % RIM, cols - RIM, RIM)
            return carry

        lax.fori_loop(0, slots, body, 0)

    def flush(p):
        return pltpu.make_async_copy(acc.at[p], grad.at[p], sem_grad.at[p])

    plane(0)
    flush(0).start()
    entry_in.wait()
    entry_out.start()
    plane(1)
    flush(1).start()
    entry_out.wait()
    flush(0).wait()
    flush(1).wait()


def pipeline_kernel(sections, tiles, counts, own, to_left, to_right, hbm_probe, hbm_phase, hbm_measured,
                    ef_hi, ef_lo, ei_hi, ei_lo, of_hi, of_lo, oi_hi, oi_lo, sort, unsort,
                    adjoint_out, contrib_out, from_left, from_right,
                    probe, phase, measured,
                    windows, left_rim, right_rim, arrived, leaving, backed, adjoint, contrib,
                    lefts, rights, turn, talls, wides, freq, spectrum,
                    sem_in, sem_own, sem_out, send_f, recv_f, send_b, recv_b,
                    send_rim, recv_rim, send_got, recv_got, token):
    g = lax.axis_index("cuts")
    t = lax.axis_index("tile")
    last = sections - 1
    mid = last - 1
    end = tiles - 1
    slots, _, extent, _ = windows.shape
    h = extent // 2
    partner = t + 1 - 2 * (t % 2)

    loads = [
        pltpu.make_async_copy(src, dst, sem_in.at[i])
        for i, (src, dst) in enumerate(
            ((hbm_phase, phase), (hbm_probe, probe), (hbm_measured, measured)))
    ]

    def own_part(s):
        return pltpu.make_async_copy(own.at[s], windows.at[s], sem_own.at[s])

    barrier = pltpu.get_barrier_semaphore()

    @pl.when(g > 0)
    def _():
        pl.semaphore_signal(barrier, inc=1, device_id={"cuts": g - 1}, device_id_type=MESH)

    @pl.when(g < last)
    def _():
        pl.semaphore_signal(barrier, inc=1, device_id={"cuts": g + 1}, device_id_type=MESH)

    @pl.when(t > 0)
    def _():
        pl.semaphore_signal(barrier, inc=1, device_id={"tile": t - 1}, device_id_type=MESH)

    @pl.when(t < end)
    def _():
        pl.semaphore_signal(barrier, inc=1, device_id={"tile": t + 1}, device_id_type=MESH)

    def exact(x, y):
        return jnp.dot(x, y, preferred_element_type=jnp.float32)

    def each(action):
        def body(s, carry):
            action(s)
            return carry

        lax.fori_loop(0, slots, body, 0)

    for load in loads:
        load.start()
    each(lambda s: own_part(s).start())

    forms = ((ef_hi, ef_lo, ei_hi, ei_lo), (of_hi, of_lo, oi_hi, oi_lo))
    for parity in range(2):
        fh, fl, ih, il = forms[parity]
        for inverse, (lh, ll, rh, rl) in enumerate(((fh, fl, ih, il), (ih, il, fh, fl))):
            at = 2 * inverse + parity
            lefts[at, :, :extent] = lh[...]
            lefts[at, :, extent : 2 * extent] = lh[...]
            lefts[at, :, 2 * extent :] = ll[...]
            rights[at, :extent] = rh[...]
            rights[at, extent : 2 * extent] = rh[...]
            rights[at, 2 * extent :] = rl[...]

    peers = (g + last - 1) // last + 1 - g // last + (t + end - 1) // end + 1 - t // end
    pl.semaphore_wait(barrier, peers)

    def rim_copy(side, s):
        src, dst = ((to_left, right_rim), (to_right, left_rim))[side]
        return pltpu.make_async_remote_copy(
            src_ref=src.at[s], dst_ref=dst.at[s], send_sem=send_rim.at[side, s],
            recv_sem=recv_rim.at[side, s], device_id={"tile": t + (-1, 1)[side]},
            device_id_type=MESH)

    def got_copy(side, s):
        start, dst = ((0, from_right), (extent - RIM, from_left))[side]
        return pltpu.make_async_remote_copy(
            src_ref=contrib.at[s, :, :, pl.ds(start, RIM)], dst_ref=dst.at[s],
            send_sem=send_got.at[side, s], recv_sem=recv_got.at[side, s],
            device_id={"tile": t + (-1, 1)[side]}, device_id_type=MESH)

    @pl.when(t > 0)
    def _():
        each(lambda s: rim_copy(0, s).start())

    @pl.when(t < end)
    def _():
        each(lambda s: rim_copy(1, s).start())

    @pl.when(t == 0)
    def _():
        left_rim[...] = jnp.zeros(left_rim.shape, left_rim.dtype)

    @pl.when(t == end)
    def _():
        right_rim[...] = jnp.zeros(right_rim.shape, right_rim.dtype)

    loads[0].wait()
    rest = phase[...]
    total = jnp.zeros((extent, extent), jnp.float32)
    for _ in range(3):
        part = rest.astype(jnp.bfloat16)
        rest = rest - part.astype(jnp.float32)
        total += exact(exact(sort[...], part).astype(jnp.bfloat16), unsort[...])
    turn[0] = jnp.cos(total)
    sine = jnp.sin(total)
    turn[1] = sine
    turn[2] = -sine
    loads[1].wait()
    loads[2].wait()

    def split(value):
        hi = value.astype(jnp.bfloat16)
        lo = (value - hi.astype(jnp.float32)).astype(jnp.bfloat16)
        return (hi, lo, hi)

    def put_tall(parity, p, value):
        for at, part in enumerate(split(value)):
            talls[parity, pl.ds(at * extent + p * h, h), :] = part

    def put_wide(parity, rows, p, value):
        n = value.shape[0]
        for at, part in enumerate(split(value)):
            wides[parity, pl.ds(rows, n), pl.ds(at * extent + p * h, h)] = part

    def left(at):
        return exact(lefts[at], talls[at % 2])

    def right(at):
        return exact(wides[at % 2], rights[at])

    def to_freq():
        for p in range(2):
            put_tall(0, p, spectrum[p, :h] + spectrum[p, h:])
            put_tall(1, p, spectrum[p, :h] - spectrum[p, h:])
        for block in range(2):
            half = left(block)
            for p in range(2):
                value = half[p * h : (p + 1) * h]
                put_wide(0, block * h, p, value[:, :h] + value[:, h:])
                put_wide(1, block * h, p, value[:, :h] - value[:, h:])
        for parity in range(2):
            freq[parity] = right(parity)

    def from_freq():
        u, v = right(2), right(3)
        for p in range(2):
            up, vp = u[:, p * h : (p + 1) * h], v[:, p * h : (p + 1) * h]
            plus, minus = up + vp, up - vp
            for parity in range(2):
                rows = slice(parity * h, (parity + 1) * h)
                both = jnp.concatenate([plus[rows], minus[rows]], axis=1)
                put_tall(parity, p, both)
        u, v = left(2), left(3)
        for p in range(2):
            up, vp = u[p * h : (p + 1) * h], v[p * h : (p + 1) * h]
            spectrum[p, :h] = up + vp
            spectrum[p, h:] = up - vp

    def send_forward(s, part):
        return pltpu.make_async_remote_copy(
            src_ref=leaving.at[s, part], dst_ref=arrived.at[s, part], send_sem=send_f.at[s, part],
            recv_sem=recv_f.at[s, part], device_id={"cuts": g + 1}, device_id_type=MESH)

    def send_backward(s):
        return pltpu.make_async_remote_copy(
            src_ref=adjoint.at[s], dst_ref=backed.at[s], send_sem=send_b.at[s],
            recv_sem=recv_b.at[s], device_id={"cuts": g - 1}, device_id_type=MESH)

    def send_window(s):
        return pltpu.make_async_remote_copy(
            src_ref=windows.at[s], dst_ref=backed.at[s], send_sem=send_b.at[s],
            recv_sem=recv_b.at[s], device_id={"cuts": g - 1}, device_id_type=MESH)

    def compose(s):
        own_part(s).wait()

        @pl.when(t < end)
        def _():
            rim_copy(0, s).wait_recv()

        @pl.when(t > 0)
        def _():
            rim_copy(1, s).wait_recv()

        for p in range(2):
            windows[s, p, :, :RIM] += left_rim[s, p]
            windows[s, p, :, extent - RIM :] += right_rim[s, p]

    def put_out(j, s):
        src, dst = ((adjoint, adjoint_out), (contrib, contrib_out))[j]
        return pltpu.make_async_copy(src.at[s], dst.at[s], sem_out.at[j, s])

    def product(w, x, s, sign):
        wr, wi = w[s, 0], w[s, 1]
        xr, xi = x
        spectrum[0] = wr * xr - sign * (wi * xi)
        spectrum[1] = wr * xi + sign * (wi * xr)

    @pl.when(g == last)
    def _():
        def body(s):
            compose(s)
            send_window(s).start()

        each(body)

    def event(s, op):
        @pl.when(op == 0)
        def _():
            @pl.when(g == 0)
            def _():
                arrived[s] = probe[...] * jnp.clip(counts[0] - s, 0, 1).astype(jnp.float32)

            @pl.when(g > 0)
            def _():
                send_forward(s, 0).wait_recv()
                send_forward(s, 1).wait_recv()

            @pl.when(g < last)
            def _():
                compose(s)

            product(windows, (arrived[s, 0], arrived[s, 1]), s, 1.0)

        @pl.when(op == 1)
        def _():
            send_window(s).wait_recv()
            product(backed, (spectrum[0], spectrum[1]), s, 1.0)

        @pl.when((op == 4) & (g < mid))
        def _():
            send_backward(s).wait_recv()
            spectrum[...] = backed[s]

        @pl.when((op == 4) & (g == mid))
        def _():
            product(backed, (spectrum[0], spectrum[1]), s, -1.0)

        to_freq()

        @pl.when(op == 2)
        def _():
            seen = exact(sort[...], measured[s]).astype(jnp.bfloat16)
            seen = exact(seen, unsort[...])
            for parity in range(2):
                fr, fi = freq[parity, :, :h], freq[parity, :, h:]
                residual = fr * fr + fi * fi - seen[:, parity * h : (parity + 1) * h]
                put_wide(parity, 0, 0, fr * residual)
                put_wide(parity, 0, 1, fi * residual)

        @pl.when(op != 2)
        def _():
            sine = 1 + op // 3
            for parity in range(2):
                cols = slice(parity * h, (parity + 1) * h)
                kr, ki = turn[0, :, cols], turn[sine, :, cols]
                xr, xi = freq[parity, :, :h], freq[parity, :, h:]
                put_wide(parity, 0, 0, kr * xr - ki * xi)
                put_wide(parity, 0, 1, kr * xi + ki * xr)

        from_freq()

        @pl.when((op == 0) & (g < last))
        def _():
            leaving[s] = spectrum[...]

            @pl.when((g == 0) & ((s > 0) | (t % 2 == 1)))
            def _():
                pl.semaphore_wait(token, 1)

            send_forward(s, 0).start()
            send_forward(s, 1).start()

            @pl.when(g == 0)
            def _():
                send_forward(s, 0).wait_send()

                @pl.when((s < slots - 1) | (t % 2 == 0))
                def _():
                    pl.semaphore_signal(token, inc=1, device_id={"tile": partner}, device_id_type=MESH)

        @pl.when(((op == 3) & (g == last)) | (op == 4))
        def _():
            tr, ti = spectrum[0], spectrum[1]
            wr, wi = windows[s, 0], windows[s, 1]
            adjoint[s, 0] = wr * tr + wi * ti
            adjoint[s, 1] = wr * ti - wi * tr

            @pl.when((g > 0) & (g < last))
            def _():
                send_backward(s).start()

            xr, xi = arrived[s, 0], arrived[s, 1]
            contrib[s, 0] = xr * tr + xi * ti
            contrib[s, 1] = xr * ti - xi * tr
            put_out(0, s).start()
            put_out(1, s).start()

            @pl.when(t > 0)
            def _():
                got_copy(0, s).start()

            @pl.when(t < end)
            def _():
                got_copy(1, s).start()

    lag = 2 * (mid - g)
    early = (g < mid).astype(jnp.int32)
    final = g // last
    ops = 5 - 3 * early - 2 * final
    count = (slots + early * lag) * ops

    def step(e, carry):
        k, part = e // ops, e % ops
        s = k - early * part * lag
        op = part + early * part * 3 + final * ((part + 1) // 2)

        @pl.when((s >= 0) & (s < slots))
        def _():
            event(s, op)

        return carry

    lax.fori_loop(0, count, step, 0)

    @pl.when(g < last)
    def _():
        each(lambda s: send_forward(s, 1).wait_send())

    @pl.when((g > 0) & (g < last))
    def _():
        each(lambda s: send_forward(s, 0).wait_send())
        each(lambda s: send_backward(s).wait_send())

    @pl.when(g == last)
    def _():
        each(lambda s: send_window(s).wait_send())

    @pl.when(t < end)
    def _():
        each(lambda s: got_copy(0, s).wait_recv())

    @pl.when(t > 0)
    def _():
        each(lambda s: got_copy(1, s).wait_recv())

    def finish(side):
        def body(s):
            rim_copy(side, s).wait_send()
            got_copy(side, s).wait_send()

        each(body)

    @pl.when(t > 0)
    def _():
        finish(0)

    @pl.when(t < end)
    def _():
        finish(1)

    each(lambda s: put_out(0, s).wait())
    each(lambda s: put_out(1, s).wait())


def on_device(probe_wave, transmission, kernel_phase, measured, counts, positions, widths):
    f32 = jnp.float32
    bf16 = jnp.bfloat16
    rows, cols = transmission.shape[2:]
    extent = probe_wave.shape[-1]
    slots = positions.shape[1]
    sections = lax.axis_size("cuts")
    tiles = lax.axis_size("tile")
    assert extent == cols and extent >= 2 * RIM and tiles % 2 == 0 and sections >= 2
    own_pos = jnp.concatenate([jnp.swapaxes(positions[0], 0, 1), widths.reshape(2, 1)], 1)
    right_pos = shift(own_pos, "tile", -1)
    left_pos = shift(own_pos, "tile", 1)
    sds = jax.ShapeDtypeStruct
    wave = sds((slots, 2, extent, extent), f32)
    rim = sds((slots, 2, extent, RIM), f32)
    waves = pltpu.VMEM(wave.shape, f32)
    rims = pltpu.VMEM(rim.shape, f32)
    hbm = pl.BlockSpec(memory_space=pl.ANY)
    dma = pltpu.SemaphoreType.DMA
    tall = extent + PAD
    own, to_left, to_right = pl.pallas_call(
        extract_kernel,
        out_shape=(wave, rim, rim),
        in_specs=[smem()] * 3 + [hbm],
        out_specs=(hbm,) * 3,
        scratch_shapes=[
            pltpu.VMEM((slots, 2, tall, RIM), f32),
            pltpu.VMEM((slots, 2, tall, RIM), f32),
            pltpu.VMEM((slots, 2, tall, cols), f32),
            rims, rims, waves,
            dma((3, slots)), dma((3, slots)),
        ],
        compiler_params=params(EXTRACT_VMEM),
    )(left_pos, right_pos, own_pos, transmission[0])
    adjoint, contrib, from_left, from_right = pl.pallas_call(
        functools.partial(pipeline_kernel, sections, tiles),
        out_shape=(wave, wave, rim, rim),
        in_specs=[smem()] + [hbm] * 6 + [vmem()] * 10,
        out_specs=(hbm,) * 4,
        scratch_shapes=[
            pltpu.VMEM((2, extent, extent), f32),
            pltpu.VMEM((extent, extent), f32),
            pltpu.VMEM((slots, extent, extent), bf16),
            waves, rims, rims,
            waves, waves, waves, waves, waves,
            pltpu.VMEM((4, extent, 3 * extent), bf16),
            pltpu.VMEM((4, 3 * extent, extent), bf16),
            pltpu.VMEM((3, extent, extent), f32),
            pltpu.VMEM((2, 3 * extent, extent), bf16),
            pltpu.VMEM((2, extent, 3 * extent), bf16),
            pltpu.VMEM((2, extent, extent), f32),
            pltpu.VMEM((2, extent, extent), f32),
            dma((3,)),
            dma((slots,)),
            dma((2, slots)),
            dma((slots, 2)), dma((slots, 2)),
            dma((slots,)), dma((slots,)),
            dma((2, slots)), dma((2, slots)),
            dma((2, slots)), dma((2, slots)),
            pltpu.SemaphoreType.REGULAR,
        ],
        compiler_params=params(PIPELINE_VMEM, collective_id=0, has_side_effects=True),
    )(counts, own, to_left, to_right, probe_wave, kernel_phase, measured[0], *make_tables(extent))
    grad, entry = pl.pallas_call(
        gather_kernel,
        out_shape=(sds((2, rows, cols), f32), wave),
        in_specs=[smem()] * 3 + [hbm] * 4,
        out_specs=(hbm, hbm),
        scratch_shapes=[
            pltpu.VMEM((2, rows, cols), f32), waves, rims, rims, waves,
            dma((3, slots)), dma((2,)), dma((2,)),
        ],
        compiler_params=params(GATHER_VMEM),
    )(left_pos, right_pos, own_pos, contrib, from_left, from_right, adjoint)
    return (entry[None, None], grad[None])


def solution(mesh):
    return jax.shard_map(
        on_device,
        mesh=mesh,
        in_specs=(
            P(),
            P("cuts", None, None, "tile"),
            P(),
            P("tile", None, None, None),
            P("tile"),
            P("tile", None, None),
            P("tile", None),
        ),
        out_specs=(P("cuts", "tile", None, None, None, None), P("cuts", None, None, "tile")),
        check_vma=False,
    )
```

```python
import functools
import math

import jax
import jax.numpy as jnp
import numpy as np
from jax import lax
from jax.experimental import pallas as pl
from jax.experimental.pallas import tpu as pltpu
from jax.sharding import PartitionSpec as P

RIM = 128
PAD = 8
MESH = pl.DeviceIdType.MESH
MIB = 1024 * 1024
EXTRACT_VMEM = 62 * MIB
PIPELINE_VMEM = 62 * MIB
GATHER_VMEM = 62 * MIB


def params(limit, **kw):
    return pltpu.CompilerParams(vmem_limit_bytes=limit, **kw)


def vmem():
    return pl.BlockSpec(memory_space=pltpu.VMEM)


def smem():
    return pl.BlockSpec(memory_space=pltpu.SMEM)


def shift(value, axis, by):
    count = lax.axis_size(axis)
    pairs = [(i, i + by) for i in range(count) if 0 <= i + by < count]
    return lax.ppermute(value, axis, pairs)


def make_tables(extent):
    half = extent // 2
    indices = np.arange(extent)
    angles = (indices[:, None] * indices[None, :] % extent) * (2.0 * math.pi / extent)
    cosine = (np.cos(angles) / math.sqrt(extent)).astype(np.float32)
    sine = (np.sin(angles) / math.sqrt(extent)).astype(np.float32)
    tables = []
    for parity in range(2):
        c, s = cosine[parity::2, :half], sine[parity::2, :half]
        block = np.block([[c, s], [-s, c]])
        for matrix in (block, block.T):
            hi = matrix.astype(jnp.bfloat16)
            lo = (matrix - hi.astype(np.float32)).astype(jnp.bfloat16)
            tables += [jnp.asarray(hi), jnp.asarray(lo)]
    order = np.concatenate([indices[0::2], indices[1::2]])
    sort = (order[:, None] == indices[None, :]).astype(jnp.bfloat16)
    return tables + [jnp.asarray(sort), jnp.asarray(np.ascontiguousarray(sort.T))]


def aligned(row, limit):
    base = jnp.minimum(row // PAD * PAD, limit)
    return pl.multiple_of(base, PAD), row - base


def extract_kernel(left_pos, right_pos, own_pos, trans, own, to_left, to_right,
                   buf_left, buf_right, buf_own, out_left, out_right, out_own, sem_in, sem_out):
    t = lax.axis_index("tile")
    end = lax.axis_size("tile") - 1
    slots, _, extent, _ = own.shape
    rows, cols = trans.shape[1:]
    tall = extent + PAD
    slack = cols + 2 * RIM - extent
    jobs = (
        (left_pos, buf_left, 0, RIM, out_left, to_left),
        (right_pos, buf_right, cols - RIM, RIM, out_right, to_right),
        (own_pos, buf_own, 0, cols, out_own, own),
    )

    def fetch(j, s):
        pos, buf, start, width = jobs[j][:4]
        base, off = aligned(pos[0, s], rows - tall)
        src = trans.at[:, pl.ds(base, tall), pl.ds(start, width)]
        return pltpu.make_async_copy(src, buf.at[s], sem_in.at[j, s]), off

    def flush(j, s):
        return pltpu.make_async_copy(jobs[j][4].at[s], jobs[j][5].at[s], sem_out.at[j, s])

    for s in range(slots):
        for j in range(3):
            fetch(j, s)[0].start()

    def columns(width):
        return lax.broadcasted_iota(jnp.int32, (extent, width), 1)

    def load(j, s, p, off, turn):
        value = pltpu.roll(jobs[j][1][s, p], (tall - off) % tall, 0)[:extent]
        return pltpu.roll(value, turn, 1)

    def body(s, carry):
        one, off = fetch(0, s)
        one.wait()
        short = slack - left_pos[1, s]
        at = columns(RIM) - short
        good = (at >= 0) & (at + 1 <= left_pos[1, slots])
        for p in range(2):
            out_left[s, p] = jnp.where(good, load(0, s, p, off, short % RIM), 0.0)
        flush(0, s).start()
        one, off = fetch(1, s)
        one.wait()
        col = right_pos[1, s]
        at = columns(RIM) + col
        good = (at < RIM) & (RIM - at <= right_pos[0, slots])
        for p in range(2):
            out_right[s, p] = jnp.where(good, load(1, s, p, off, (cols - col) % RIM), 0.0)
        flush(1, s).start()
        one, off = fetch(2, s)
        one.wait()
        col = own_pos[1, s]
        at = columns(extent) + col
        middle = (at >= RIM) & (at < RIM + cols)
        left_ok = (t > 0) & (at < RIM) & (RIM - at <= own_pos[0, slots])
        right_ok = (t < end) & (at >= RIM + cols) & (at - RIM - cols + 1 <= own_pos[1, slots])
        rim = left_ok | right_ok
        for p in range(2):
            value = load(2, s, p, off, (cols + RIM - col) % cols)
            out_own[s, p] = jnp.where(middle, value, jnp.where(rim, 0.0, 1.0 - p))
        flush(2, s).start()
        return carry

    lax.fori_loop(0, slots, body, 0)
    for s in range(slots):
        for j in range(3):
            flush(j, s).wait()


def gather_kernel(left_pos, right_pos, own_pos, contrib, from_left,
                  from_right, adjoint, grad, entry, acc, buf_own, buf_left, buf_right, buf_entry,
                  sem_in, sem_entry, sem_grad):
    slots, _, extent, _ = buf_own.shape
    rows, cols = acc.shape[1:]
    tall = extent + PAD
    slack = cols + 2 * RIM - extent
    jobs = ((contrib, buf_own), (from_left, buf_left), (from_right, buf_right))

    def fetch(j, s):
        return pltpu.make_async_copy(jobs[j][0].at[s], jobs[j][1].at[s], sem_in.at[j, s])

    for s in range(slots):
        for j in range(3):
            fetch(j, s).start()
    entry_in = pltpu.make_async_copy(adjoint, buf_entry, sem_entry.at[0])
    entry_out = pltpu.make_async_copy(buf_entry, entry, sem_entry.at[1])
    entry_in.start()
    acc[...] = jnp.zeros(acc.shape, acc.dtype)

    def columns(width):
        return lax.broadcasted_iota(jnp.int32, (extent, width), 1)

    def add(source, s, p, row, good, turn, start, width):
        base, off = aligned(row, rows - tall)
        value = jnp.where(good, pltpu.roll(source[s, p], turn, 1), 0.0)
        value = jnp.concatenate([value, jnp.zeros((PAD, width), jnp.float32)], axis=0)
        acc[p, pl.ds(base, tall), pl.ds(start, width)] += pltpu.roll(value, off, 0)

    def plane(p):
        def body(s, carry):
            if p == 0:
                for j in range(3):
                    fetch(j, s).wait()
            col = own_pos[1, s]
            at = columns(cols) + RIM - col
            good = (at >= 0) & (at < extent)
            add(buf_own, s, p, own_pos[0, s], good, (col + cols - RIM) % cols, 0, cols)
            short = slack - left_pos[1, s]
            at = columns(RIM)
            good = (at + short < RIM) & (at + 1 <= left_pos[1, slots])
            add(buf_left, s, p, left_pos[0, s], good, (cols - short) % RIM, 0, RIM)
            col = right_pos[1, s]
            good = (at >= col) & (RIM - at <= right_pos[0, slots])
            add(buf_right, s, p, right_pos[0, s], good, col % RIM, cols - RIM, RIM)
            return carry

        lax.fori_loop(0, slots, body, 0)

    def flush(p):
        return pltpu.make_async_copy(acc.at[p], grad.at[p], sem_grad.at[p])

    plane(0)
    flush(0).start()
    entry_in.wait()
    entry_out.start()
    plane(1)
    flush(1).start()
    entry_out.wait()
    flush(0).wait()
    flush(1).wait()


ENTER, BEYOND, WHOLE, BACK, OFFER, RELAY = range(1, 7)


def schedule(g, last, slots):
    mid, alone = last - 1, slots - 1
    relays = [(0, RELAY, m) for m in range(g + 1, last + 1)]
    plan = [(0, OFFER, g)] * (0 < g < last)
    if g >= mid:
        return plan + relays + [(s, WHOLE, g) for s in range(slots)]
    lag = 2 * (mid - g)
    done = 0
    for k in range(slots):
        plan += [(k, ENTER, g)]
        if g > 0 and relays:
            plan += [relays.pop(0)]
        if k >= lag:
            plan += [(done, BACK, g)]
            done += 1
    while done < alone - 2:
        plan += [(done, BACK, g)]
        done += 1
    plan += relays + [(alone, BEYOND, g)]
    while done < alone:
        plan += [(done, BACK, g)]
        done += 1
    return plan


def pipeline_kernel(sections, tiles, counts, own, to_left, to_right, hbm_probe, hbm_phase, hbm_measured,
                    ef_hi, ef_lo, ei_hi, ei_lo, of_hi, of_lo, oi_hi, oi_lo, sort, unsort,
                    adjoint_out, contrib_out, from_left, from_right,
                    probe, phase, measured,
                    windows, left_rim, right_rim, arrived, leaving, backed, adjoint, contrib,
                    lefts, rights, turn, talls, wides, spectrum,
                    sem_in, sem_own, sem_out, send_f, recv_f, send_b, recv_b, send_far, recv_far,
                    send_rim, recv_rim, send_got, recv_got, token):
    g = lax.axis_index("cuts")
    t = lax.axis_index("tile")
    last = sections - 1
    mid = last - 1
    end = tiles - 1
    slots, _, extent, _ = windows.shape
    h = extent // 2
    partner = t + 1 - 2 * (t % 2)
    alone = slots - 1

    loads = [
        pltpu.make_async_copy(src, dst, sem_in.at[i])
        for i, (src, dst) in enumerate(
            ((hbm_phase, phase), (hbm_probe, probe), (hbm_measured, measured)))
    ]

    def own_part(s):
        return pltpu.make_async_copy(own.at[s], windows.at[s], sem_own.at[s])

    barrier = pltpu.get_barrier_semaphore()

    @pl.when(g > 0)
    def _():
        pl.semaphore_signal(barrier, inc=1, device_id={"cuts": g - 1}, device_id_type=MESH)

    @pl.when(g < last)
    def _():
        pl.semaphore_signal(barrier, inc=1, device_id={"cuts": g + 1}, device_id_type=MESH)

    @pl.when(t > 0)
    def _():
        pl.semaphore_signal(barrier, inc=1, device_id={"tile": t - 1}, device_id_type=MESH)

    @pl.when(t < end)
    def _():
        pl.semaphore_signal(barrier, inc=1, device_id={"tile": t + 1}, device_id_type=MESH)

    def exact(x, y):
        return jnp.dot(x, y, preferred_element_type=jnp.float32)

    def each(action):
        def body(s, carry):
            action(s)
            return carry

        lax.fori_loop(0, slots, body, 0)

    for load in loads:
        load.start()
    each(lambda s: own_part(s).start())

    def turn_of(i):
        return (i + alone * ((g + last - 1) // last)) % slots

    forms = ((ef_hi, ef_lo, ei_hi, ei_lo), (of_hi, of_lo, oi_hi, oi_lo))
    for parity in range(2):
        fh, fl, ih, il = forms[parity]
        for inverse, (lh, ll, rh, rl) in enumerate(((fh, fl, ih, il), (ih, il, fh, fl))):
            at = 2 * inverse + parity
            lefts[at, :, :extent] = lh[...]
            lefts[at, :, extent : 2 * extent] = lh[...]
            lefts[at, :, 2 * extent :] = ll[...]
            rights[at, :extent] = rh[...]
            rights[at, extent : 2 * extent] = rh[...]
            rights[at, 2 * extent :] = rl[...]

    peers = (g + last - 1) // last + 1 - g // last + (t + end - 1) // end + 1 - t // end
    pl.semaphore_wait(barrier, peers)

    def rim_copy(side, s):
        src, dst = ((to_left, right_rim), (to_right, left_rim))[side]
        return pltpu.make_async_remote_copy(
            src_ref=src.at[s], dst_ref=dst.at[s], send_sem=send_rim.at[side, s],
            recv_sem=recv_rim.at[side, s], device_id={"tile": t + (-1, 1)[side]},
            device_id_type=MESH)

    def got_copy(side, s):
        start, dst = ((0, from_right), (extent - RIM, from_left))[side]
        return pltpu.make_async_remote_copy(
            src_ref=contrib.at[s, :, :, pl.ds(start, RIM)], dst_ref=dst.at[s],
            send_sem=send_got.at[side, s], recv_sem=recv_got.at[side, s],
            device_id={"tile": t + (-1, 1)[side]}, device_id_type=MESH)

    def rims_start(i):
        s = turn_of(i)

        @pl.when(t > 0)
        def _():
            rim_copy(0, s).start()

        @pl.when(t < end)
        def _():
            rim_copy(1, s).start()

    each(rims_start)

    @pl.when(t == 0)
    def _():
        left_rim[...] = jnp.zeros(left_rim.shape, left_rim.dtype)

    @pl.when(t == end)
    def _():
        right_rim[...] = jnp.zeros(right_rim.shape, right_rim.dtype)

    loads[0].wait()
    rest = phase[...]
    total = jnp.zeros((extent, extent), jnp.float32)
    for _ in range(3):
        part = rest.astype(jnp.bfloat16)
        rest = rest - part.astype(jnp.float32)
        total += exact(exact(sort[...], part).astype(jnp.bfloat16), unsort[...])
    turn[0] = jnp.cos(total)
    sine = jnp.sin(total)
    turn[1] = sine
    turn[2] = -sine
    loads[1].wait()
    loads[2].wait()

    def split(value):
        hi = value.astype(jnp.bfloat16)
        lo = (value - hi.astype(jnp.float32)).astype(jnp.bfloat16)
        return (hi, lo, hi)

    def put_tall(parity, p, value):
        for at, part in enumerate(split(value)):
            talls[parity, pl.ds(at * extent + p * h, h), :] = part

    def put_wide(parity, rows, p, value):
        n = value.shape[0]
        for at, part in enumerate(split(value)):
            wides[parity, pl.ds(rows, n), pl.ds(at * extent + p * h, h)] = part

    def left(at):
        return exact(lefts[at], talls[at % 2])

    def right(at):
        return exact(wides[at % 2], rights[at])

    def halves(load):
        upper, lower = load(slice(0, h)), load(slice(h, extent))
        for p in range(2):
            put_tall(0, p, upper[p] + lower[p])
            put_tall(1, p, upper[p] - lower[p])

    def plain(ref, *at):
        def load(rows):
            return [ref[(*at, p, rows)] for p in range(2)]

        return load

    def through(w, w_at, x, x_at, sign):
        def load(rows):
            wr, wi = w[w_at, 0, rows], w[w_at, 1, rows]
            xr, xi = x[(*x_at, 0, rows)], x[(*x_at, 1, rows)]
            if sign > 0:
                return [wr * xr - wi * xi, wr * xi + wi * xr]
            return [wr * xr + wi * xi, wr * xi - wi * xr]

        return load

    def turned(sine):
        def middle(parity, xr, xi):
            cols = slice(parity * h, (parity + 1) * h)
            kr, ki = turn[0, :, cols], turn[sine, :, cols]
            return kr * xr - ki * xi, kr * xi + ki * xr

        return middle

    def transform(load, middle):
        halves(load)
        for block in range(2):
            half = left(block)
            for p in range(2):
                value = half[p * h : (p + 1) * h]
                put_wide(0, block * h, p, value[:, :h] + value[:, h:])
                put_wide(1, block * h, p, value[:, :h] - value[:, h:])
        for parity in range(2):
            value = right(parity)
            for p, part in enumerate(middle(parity, value[:, :h], value[:, h:])):
                put_wide(parity, 0, p, part)
        u, v = right(2), right(3)
        for p in range(2):
            up, vp = u[:, p * h : (p + 1) * h], v[:, p * h : (p + 1) * h]
            plus, minus = up + vp, up - vp
            for parity in range(2):
                rows = slice(parity * h, (parity + 1) * h)
                put_tall(parity, p, jnp.concatenate([plus[rows], minus[rows]], axis=1))
        u, v = left(2), left(3)
        for p in range(2):
            up, vp = u[p * h : (p + 1) * h], v[p * h : (p + 1) * h]
            spectrum[p, :h] = up + vp
            spectrum[p, h:] = up - vp

    def send_forward(s, part):
        return pltpu.make_async_remote_copy(
            src_ref=leaving.at[s, part], dst_ref=arrived.at[s, part], send_sem=send_f.at[s, part],
            recv_sem=recv_f.at[s, part], device_id={"cuts": g + 1}, device_id_type=MESH)

    def send_backward(s):
        return pltpu.make_async_remote_copy(
            src_ref=adjoint.at[s], dst_ref=backed.at[s], send_sem=send_b.at[s],
            recv_sem=recv_b.at[s], device_id={"cuts": g - 1}, device_id_type=MESH)

    def send_window(s):
        return pltpu.make_async_remote_copy(
            src_ref=windows.at[s], dst_ref=backed.at[s], send_sem=send_b.at[s],
            recv_sem=recv_b.at[s], device_id={"cuts": g - 1}, device_id_type=MESH)

    def far_at(m):
        return slots + m - 1

    def send_own_far():
        return pltpu.make_async_remote_copy(
            src_ref=windows.at[alone], dst_ref=backed.at[far_at(g)], send_sem=send_far.at[g],
            recv_sem=recv_far.at[g], device_id={"cuts": g - 1}, device_id_type=MESH)

    def send_far_on(m):
        return pltpu.make_async_remote_copy(
            src_ref=backed.at[far_at(m)], dst_ref=backed.at[far_at(m)], send_sem=send_far.at[m],
            recv_sem=recv_far.at[m], device_id={"cuts": g - 1}, device_id_type=MESH)

    def compose(s):
        own_part(s).wait()

        @pl.when(t < end)
        def _():
            rim_copy(0, s).wait_recv()

        @pl.when(t > 0)
        def _():
            rim_copy(1, s).wait_recv()

        for p in range(2):
            windows[s, p, :, :RIM] += left_rim[s, p]
            windows[s, p, :, extent - RIM :] += right_rim[s, p]

    def put_out(j, s):
        src, dst = ((adjoint, adjoint_out), (contrib, contrib_out))[j]
        return pltpu.make_async_copy(src.at[s], dst.at[s], sem_out.at[j, s])

    @pl.when(g == last)
    def _():
        def body(i):
            s = turn_of(i)
            compose(s)

            @pl.when(s == alone)
            def _():
                send_own_far().start()

            @pl.when(s < alone)
            def _():
                send_window(s).start()

        each(body)

    def enter(s):
        @pl.when(g == 0)
        def _():
            arrived[s] = probe[...] * jnp.clip(counts[0] - s, 0, 1).astype(jnp.float32)

        @pl.when(g > 0)
        def _():
            send_forward(s, 0).wait_recv()
            send_forward(s, 1).wait_recv()

        @pl.when((g < last) & ((g == 0) | (s < alone)))
        def _():
            compose(s)

        transform(through(windows, s, arrived, (s,), 1), turned(1))

        @pl.when(g < last)
        def _():
            leaving[s] = spectrum[...]

            @pl.when((g == 0) & ((s > 0) | (t % 2 == 1)))
            def _():
                pl.semaphore_wait(token, 1)

            send_forward(s, 0).start()
            send_forward(s, 1).start()

            @pl.when(g == 0)
            def _():
                send_forward(s, 0).wait_send()

                @pl.when((s < slots - 1) | (t % 2 == 0))
                def _():
                    pl.semaphore_signal(token, inc=1, device_id={"tile": partner}, device_id_type=MESH)

    def beyond(s):
        later = last - g

        @pl.when((g == mid) & (s < alone))
        def _():
            send_window(s).wait_recv()

        @pl.when(g < mid)
        def _():
            spectrum[...] = leaving[s]

        def onward(i, carry):
            spot = jnp.where(s == alone, far_at(g + 1 + i), s)
            transform(through(backed, spot, spectrum, (), 1), turned(1))
            return carry

        lax.fori_loop(0, later, onward, 0)
        seen = exact(sort[...], measured[s]).astype(jnp.bfloat16)
        seen = exact(seen, unsort[...])

        def detected(parity, xr, xi):
            residual = xr * xr + xi * xi - seen[:, parity * h : (parity + 1) * h]
            return xr * residual, xi * residual

        transform(plain(spectrum), detected)
        transform(plain(spectrum), turned(2))

        def homeward(i, carry):
            spot = jnp.where(s == alone, far_at(last - i), s)
            transform(through(backed, spot, spectrum, (), -1), turned(2))
            return carry

        lax.fori_loop(0, later, homeward, 0)

    def back(s):
        send_backward(s).wait_recv()
        transform(plain(backed, s), turned(2))

    def finish_slot(s):
        tr, ti = spectrum[0], spectrum[1]
        wr, wi = windows[s, 0], windows[s, 1]
        adjoint[s, 0] = wr * tr + wi * ti
        adjoint[s, 1] = wr * ti - wi * tr

        @pl.when((g > 0) & (g < last) & (s < alone))
        def _():
            send_backward(s).start()

        xr, xi = arrived[s, 0], arrived[s, 1]
        contrib[s, 0] = xr * tr + xi * ti
        contrib[s, 1] = xr * ti - xi * tr

        @pl.when(t > 0)
        def _():
            got_copy(0, s).start()

        @pl.when(t < end)
        def _():
            got_copy(1, s).start()

        put_out(0, s).start()
        put_out(1, s).start()

    plans = [schedule(here, last, slots) for here in range(sections)]
    width = max(len(plan) for plan in plans)

    def step(e, carry):
        code = jnp.int32(0)
        for here, plan in enumerate(plans):
            for at, (s, act, m) in enumerate(plan):
                code = jnp.where((g == here) & (e == at), (s * 8 + act) * (sections + 1) + m + 1, code)
        m, rest = code % (sections + 1) - 1, code // (sections + 1)
        act, s = rest % 8, rest // 8

        @pl.when((act == ENTER) | (act == WHOLE))
        def _():
            enter(s)

        @pl.when((act == BEYOND) | (act == WHOLE))
        def _():
            beyond(s)

        @pl.when(act == BACK)
        def _():
            back(s)

        @pl.when((act == BEYOND) | (act == WHOLE) | (act == BACK))
        def _():
            finish_slot(s)

        @pl.when(act == OFFER)
        def _():
            compose(alone)
            send_own_far().start()

        @pl.when(act == RELAY)
        def _():
            send_far_on(m).wait_recv()

            @pl.when(g > 0)
            def _():
                send_far_on(m).start()

        return carry

    lax.fori_loop(0, width, step, 0)

    def all_but_lone(action):
        def body(s, carry):
            action(s)
            return carry

        lax.fori_loop(0, alone, body, 0)

    @pl.when(g < last)
    def _():
        each(lambda s: send_forward(s, 1).wait_send())

    @pl.when((g > 0) & (g < last))
    def _():
        each(lambda s: send_forward(s, 0).wait_send())
        all_but_lone(lambda s: send_backward(s).wait_send())

    @pl.when(g == last)
    def _():
        all_but_lone(lambda s: send_window(s).wait_send())

    @pl.when(g > 0)
    def _():
        send_own_far().wait_send()

    for m in range(2, sections):
        @pl.when((g > 0) & (g < m))
        def _():
            send_far_on(m).wait_send()

    @pl.when(t < end)
    def _():
        each(lambda s: got_copy(0, s).wait_recv())

    @pl.when(t > 0)
    def _():
        each(lambda s: got_copy(1, s).wait_recv())

    def finish(side):
        def body(s):
            rim_copy(side, s).wait_send()
            got_copy(side, s).wait_send()

        each(body)

    @pl.when(t > 0)
    def _():
        finish(0)

    @pl.when(t < end)
    def _():
        finish(1)

    each(lambda s: put_out(0, s).wait())
    each(lambda s: put_out(1, s).wait())


def on_device(probe_wave, transmission, kernel_phase, measured, counts, positions, widths):
    f32 = jnp.float32
    bf16 = jnp.bfloat16
    rows, cols = transmission.shape[2:]
    extent = probe_wave.shape[-1]
    slots = positions.shape[1]
    sections = lax.axis_size("cuts")
    tiles = lax.axis_size("tile")
    assert extent == cols and extent >= 2 * RIM and tiles % 2 == 0 and sections >= 2
    own_pos = jnp.concatenate([jnp.swapaxes(positions[0], 0, 1), widths.reshape(2, 1)], 1)
    right_pos = shift(own_pos, "tile", -1)
    left_pos = shift(own_pos, "tile", 1)
    sds = jax.ShapeDtypeStruct
    wave = sds((slots, 2, extent, extent), f32)
    rim = sds((slots, 2, extent, RIM), f32)
    waves = pltpu.VMEM(wave.shape, f32)
    rims = pltpu.VMEM(rim.shape, f32)
    hbm = pl.BlockSpec(memory_space=pl.ANY)
    dma = pltpu.SemaphoreType.DMA
    tall = extent + PAD
    own, to_left, to_right = pl.pallas_call(
        extract_kernel,
        out_shape=(wave, rim, rim),
        in_specs=[smem()] * 3 + [hbm],
        out_specs=(hbm,) * 3,
        scratch_shapes=[
            pltpu.VMEM((slots, 2, tall, RIM), f32),
            pltpu.VMEM((slots, 2, tall, RIM), f32),
            pltpu.VMEM((slots, 2, tall, cols), f32),
            rims, rims, waves,
            dma((3, slots)), dma((3, slots)),
        ],
        compiler_params=params(EXTRACT_VMEM),
    )(left_pos, right_pos, own_pos, transmission[0])
    adjoint, contrib, from_left, from_right = pl.pallas_call(
        functools.partial(pipeline_kernel, sections, tiles),
        out_shape=(wave, wave, rim, rim),
        in_specs=[smem()] + [hbm] * 6 + [vmem()] * 10,
        out_specs=(hbm,) * 4,
        scratch_shapes=[
            pltpu.VMEM((2, extent, extent), f32),
            pltpu.VMEM((extent, extent), f32),
            pltpu.VMEM((slots, extent, extent), bf16),
            waves, rims, rims,
            waves, waves,
            pltpu.VMEM((slots + sections - 1, 2, extent, extent), f32),
            waves, waves,
            pltpu.VMEM((4, extent, 3 * extent), bf16),
            pltpu.VMEM((4, 3 * extent, extent), bf16),
            pltpu.VMEM((3, extent, extent), f32),
            pltpu.VMEM((2, 3 * extent, extent), bf16),
            pltpu.VMEM((2, extent, 3 * extent), bf16),
            pltpu.VMEM((2, extent, extent), f32),
            dma((3,)),
            dma((slots,)),
            dma((2, slots)),
            dma((slots, 2)), dma((slots, 2)),
            dma((slots,)), dma((slots,)),
            dma((sections,)), dma((sections,)),
            dma((2, slots)), dma((2, slots)),
            dma((2, slots)), dma((2, slots)),
            pltpu.SemaphoreType.REGULAR,
        ],
        compiler_params=params(PIPELINE_VMEM, collective_id=0, has_side_effects=True),
    )(counts, own, to_left, to_right, probe_wave, kernel_phase, measured[0], *make_tables(extent))
    grad, entry = pl.pallas_call(
        gather_kernel,
        out_shape=(sds((2, rows, cols), f32), wave),
        in_specs=[smem()] * 3 + [hbm] * 4,
        out_specs=(hbm, hbm),
        scratch_shapes=[
            pltpu.VMEM((2, rows, cols), f32), waves, rims, rims, waves,
            dma((3, slots)), dma((2,)), dma((2,)),
        ],
        compiler_params=params(GATHER_VMEM),
    )(left_pos, right_pos, own_pos, contrib, from_left, from_right, adjoint)
    return (entry[None, None], grad[None])


def solution(mesh):
    return jax.shard_map(
        on_device,
        mesh=mesh,
        in_specs=(
            P(),
            P("cuts", None, None, "tile"),
            P(),
            P("tile", None, None, None),
            P("tile"),
            P("tile", None, None),
            P("tile", None),
        ),
        out_specs=(P("cuts", "tile", None, None, None, None), P("cuts", None, None, "tile")),
        check_vma=False,
    )
```

```python
import functools
import math

import jax
import jax.numpy as jnp
import numpy as np
from jax import lax
from jax.experimental import pallas as pl
from jax.experimental.pallas import tpu as pltpu
from jax.sharding import PartitionSpec as P

RIM = 128
PAD = 8
MESH = pl.DeviceIdType.MESH
MIB = 1024 * 1024
EXTRACT_VMEM = 62 * MIB
PIPELINE_VMEM = 62 * MIB
GATHER_VMEM = 62 * MIB


def params(limit, **kw):
    return pltpu.CompilerParams(vmem_limit_bytes=limit, **kw)


def vmem():
    return pl.BlockSpec(memory_space=pltpu.VMEM)


def smem():
    return pl.BlockSpec(memory_space=pltpu.SMEM)


def shift(value, axis, by):
    count = lax.axis_size(axis)
    pairs = [(i, i + by) for i in range(count) if 0 <= i + by < count]
    return lax.ppermute(value, axis, pairs)


def make_tables(extent):
    half = extent // 2
    indices = np.arange(extent)
    angles = (indices[:, None] * indices[None, :] % extent) * (2.0 * math.pi / extent)
    cosine = (np.cos(angles) / math.sqrt(extent)).astype(np.float32)
    sine = (np.sin(angles) / math.sqrt(extent)).astype(np.float32)
    tables = []
    for parity in range(2):
        c, s = cosine[parity::2, :half], sine[parity::2, :half]
        block = np.block([[c, s], [-s, c]])
        for matrix in (block, block.T):
            hi = matrix.astype(jnp.bfloat16)
            lo = (matrix - hi.astype(np.float32)).astype(jnp.bfloat16)
            tables += [jnp.asarray(hi), jnp.asarray(lo)]
    order = np.concatenate([indices[0::2], indices[1::2]])
    sort = (order[:, None] == indices[None, :]).astype(jnp.bfloat16)
    return tables + [jnp.asarray(sort), jnp.asarray(np.ascontiguousarray(sort.T))]


def aligned(row, limit):
    base = jnp.minimum(row // PAD * PAD, limit)
    return pl.multiple_of(base, PAD), row - base


def extract_kernel(left_pos, right_pos, own_pos, trans, own, to_left, to_right,
                   buf_left, buf_right, buf_own, out_left, out_right, out_own, sem_in, sem_out):
    t = lax.axis_index("tile")
    end = lax.axis_size("tile") - 1
    slots, _, extent, _ = own.shape
    rows, cols = trans.shape[1:]
    tall = extent + PAD
    slack = cols + 2 * RIM - extent
    jobs = (
        (left_pos, buf_left, 0, RIM, out_left, to_left),
        (right_pos, buf_right, cols - RIM, RIM, out_right, to_right),
        (own_pos, buf_own, 0, cols, out_own, own),
    )

    def fetch(j, s):
        pos, buf, start, width = jobs[j][:4]
        base, off = aligned(pos[0, s], rows - tall)
        src = trans.at[:, pl.ds(base, tall), pl.ds(start, width)]
        return pltpu.make_async_copy(src, buf.at[s], sem_in.at[j, s]), off

    def flush(j, s):
        return pltpu.make_async_copy(jobs[j][4].at[s], jobs[j][5].at[s], sem_out.at[j, s])

    for s in range(slots):
        for j in range(3):
            fetch(j, s)[0].start()

    def columns(width):
        return lax.broadcasted_iota(jnp.int32, (extent, width), 1)

    def load(j, s, p, off, turn):
        value = pltpu.roll(jobs[j][1][s, p], (tall - off) % tall, 0)[:extent]
        return pltpu.roll(value, turn, 1)

    def body(s, carry):
        one, off = fetch(0, s)
        one.wait()
        short = slack - left_pos[1, s]
        at = columns(RIM) - short
        good = (at >= 0) & (at + 1 <= left_pos[1, slots])
        for p in range(2):
            out_left[s, p] = jnp.where(good, load(0, s, p, off, short % RIM), 0.0)
        flush(0, s).start()
        one, off = fetch(1, s)
        one.wait()
        col = right_pos[1, s]
        at = columns(RIM) + col
        good = (at < RIM) & (RIM - at <= right_pos[0, slots])
        for p in range(2):
            out_right[s, p] = jnp.where(good, load(1, s, p, off, (cols - col) % RIM), 0.0)
        flush(1, s).start()
        one, off = fetch(2, s)
        one.wait()
        col = own_pos[1, s]
        at = columns(extent) + col
        middle = (at >= RIM) & (at < RIM + cols)
        left_ok = (t > 0) & (at < RIM) & (RIM - at <= own_pos[0, slots])
        right_ok = (t < end) & (at >= RIM + cols) & (at - RIM - cols + 1 <= own_pos[1, slots])
        rim = left_ok | right_ok
        for p in range(2):
            value = load(2, s, p, off, (cols + RIM - col) % cols)
            out_own[s, p] = jnp.where(middle, value, jnp.where(rim, 0.0, 1.0 - p))
        flush(2, s).start()
        return carry

    lax.fori_loop(0, slots, body, 0)
    for s in range(slots):
        for j in range(3):
            flush(j, s).wait()


def gather_kernel(left_pos, right_pos, own_pos, contrib, from_left,
                  from_right, adjoint, grad, entry, acc, buf_own, buf_left, buf_right, buf_entry,
                  sem_in, sem_entry, sem_grad):
    slots, _, extent, _ = buf_own.shape
    rows, cols = acc.shape[1:]
    tall = extent + PAD
    slack = cols + 2 * RIM - extent
    jobs = ((contrib, buf_own), (from_left, buf_left), (from_right, buf_right))

    def fetch(j, s):
        return pltpu.make_async_copy(jobs[j][0].at[s], jobs[j][1].at[s], sem_in.at[j, s])

    for s in range(slots):
        for j in range(3):
            fetch(j, s).start()
    entry_in = pltpu.make_async_copy(adjoint, buf_entry, sem_entry.at[0])
    entry_out = pltpu.make_async_copy(buf_entry, entry, sem_entry.at[1])
    entry_in.start()
    acc[...] = jnp.zeros(acc.shape, acc.dtype)

    def columns(width):
        return lax.broadcasted_iota(jnp.int32, (extent, width), 1)

    def add(source, s, p, row, good, turn, start, width):
        base, off = aligned(row, rows - tall)
        value = jnp.where(good, pltpu.roll(source[s, p], turn, 1), 0.0)
        value = jnp.concatenate([value, jnp.zeros((PAD, width), jnp.float32)], axis=0)
        acc[p, pl.ds(base, tall), pl.ds(start, width)] += pltpu.roll(value, off, 0)

    def plane(p):
        def body(s, carry):
            if p == 0:
                for j in range(3):
                    fetch(j, s).wait()
            col = own_pos[1, s]
            at = columns(cols) + RIM - col
            good = (at >= 0) & (at < extent)
            add(buf_own, s, p, own_pos[0, s], good, (col + cols - RIM) % cols, 0, cols)
            short = slack - left_pos[1, s]
            at = columns(RIM)
            good = (at + short < RIM) & (at + 1 <= left_pos[1, slots])
            add(buf_left, s, p, left_pos[0, s], good, (cols - short) % RIM, 0, RIM)
            col = right_pos[1, s]
            good = (at >= col) & (RIM - at <= right_pos[0, slots])
            add(buf_right, s, p, right_pos[0, s], good, col % RIM, cols - RIM, RIM)
            return carry

        lax.fori_loop(0, slots, body, 0)

    def flush(p):
        return pltpu.make_async_copy(acc.at[p], grad.at[p], sem_grad.at[p])

    plane(0)
    flush(0).start()
    entry_in.wait()
    entry_out.start()
    plane(1)
    flush(1).start()
    entry_out.wait()
    flush(0).wait()
    flush(1).wait()


ENTER, BEYOND, WHOLE, BACK, OFFER, RELAY = range(1, 7)


def schedule(g, last, slots):
    mid, alone = last - 1, slots - 1
    relays = [(0, RELAY, m) for m in range(g + 1, last + 1)]
    plan = [(0, OFFER, g)] * (0 < g < last)
    if g >= mid:
        return plan + relays + [(s, WHOLE, g) for s in range(slots)]
    lag = 2 * (mid - g)
    done = 0
    for k in range(slots):
        plan += [(k, ENTER, g)]
        if g > 0 and relays:
            plan += [relays.pop(0)]
        if k >= lag:
            plan += [(done, BACK, g)]
            done += 1
    while done < alone - 2:
        plan += [(done, BACK, g)]
        done += 1
    plan += relays + [(alone, BEYOND, g)]
    while done < alone:
        plan += [(done, BACK, g)]
        done += 1
    return plan


def pipeline_kernel(sections, tiles, counts, own, to_left, to_right, hbm_probe, hbm_phase, hbm_measured,
                    ef_hi, ef_lo, ei_hi, ei_lo, of_hi, of_lo, oi_hi, oi_lo, sort, unsort,
                    adjoint_out, contrib_out, from_left, from_right,
                    probe, phase, measured,
                    windows, left_rim, right_rim, arrived, leaving, backed, adjoint, contrib,
                    lefts, rights, turn, talls, wides, spectrum,
                    sem_in, sem_own, sem_out, send_f, recv_f, send_b, recv_b, send_far, recv_far,
                    send_rim, recv_rim, send_got, recv_got, token):
    g = lax.axis_index("cuts")
    t = lax.axis_index("tile")
    last = sections - 1
    mid = last - 1
    end = tiles - 1
    slots, _, extent, _ = windows.shape
    h = extent // 2
    partner = t + 1 - 2 * (t % 2)
    alone = slots - 1

    loads = [
        pltpu.make_async_copy(src, dst, sem_in.at[i])
        for i, (src, dst) in enumerate(
            ((hbm_phase, phase), (hbm_probe, probe), (hbm_measured, measured)))
    ]

    def own_part(s):
        return pltpu.make_async_copy(own.at[s], windows.at[s], sem_own.at[s])

    barrier = pltpu.get_barrier_semaphore()

    @pl.when(g > 0)
    def _():
        pl.semaphore_signal(barrier, inc=1, device_id={"cuts": g - 1}, device_id_type=MESH)

    @pl.when(g < last)
    def _():
        pl.semaphore_signal(barrier, inc=1, device_id={"cuts": g + 1}, device_id_type=MESH)

    @pl.when(t > 0)
    def _():
        pl.semaphore_signal(barrier, inc=1, device_id={"tile": t - 1}, device_id_type=MESH)

    @pl.when(t < end)
    def _():
        pl.semaphore_signal(barrier, inc=1, device_id={"tile": t + 1}, device_id_type=MESH)

    def exact(x, y):
        return jnp.dot(x, y, preferred_element_type=jnp.float32)

    def each(action):
        def body(s, carry):
            action(s)
            return carry

        lax.fori_loop(0, slots, body, 0)

    for load in loads:
        load.start()
    each(lambda s: own_part(s).start())

    def turn_of(i):
        return (i + alone * ((g + last - 1) // last)) % slots

    forms = ((ef_hi, ef_lo, ei_hi, ei_lo), (of_hi, of_lo, oi_hi, oi_lo))
    for parity in range(2):
        fh, fl, ih, il = forms[parity]
        for inverse, (lh, ll, rh, rl) in enumerate(((fh, fl, ih, il), (ih, il, fh, fl))):
            at = 2 * inverse + parity
            lefts[at, :, :extent] = lh[...]
            lefts[at, :, extent : 2 * extent] = lh[...]
            lefts[at, :, 2 * extent :] = ll[...]
            rights[at, :extent] = rh[...]
            rights[at, extent : 2 * extent] = rh[...]
            rights[at, 2 * extent :] = rl[...]

    peers = (g + last - 1) // last + 1 - g // last + (t + end - 1) // end + 1 - t // end
    pl.semaphore_wait(barrier, peers)

    def rim_copy(side, s):
        src, dst = ((to_left, right_rim), (to_right, left_rim))[side]
        return pltpu.make_async_remote_copy(
            src_ref=src.at[s], dst_ref=dst.at[s], send_sem=send_rim.at[side, s],
            recv_sem=recv_rim.at[side, s], device_id={"tile": t + (-1, 1)[side]},
            device_id_type=MESH)

    def got_copy(side, s):
        start, dst = ((0, from_right), (extent - RIM, from_left))[side]
        return pltpu.make_async_remote_copy(
            src_ref=contrib.at[s, :, :, pl.ds(start, RIM)], dst_ref=dst.at[s],
            send_sem=send_got.at[side, s], recv_sem=recv_got.at[side, s],
            device_id={"tile": t + (-1, 1)[side]}, device_id_type=MESH)

    yielding = (t % 2 == 0) & (t > 0)

    def rims_start(side, s, ok):
        @pl.when(ok)
        def _():
            rim_copy(side, s).start()

    def rims_one(i):
        s = turn_of(i)
        rims_start(0, s, (t > 0) & jnp.logical_not(yielding))
        rims_start(1, s, t < end)

    each(rims_one)

    @pl.when(yielding)
    def _():
        rim_copy(0, turn_of(0)).wait_recv()

    each(lambda i: rims_start(0, turn_of(i), yielding))

    @pl.when(t == 0)
    def _():
        left_rim[...] = jnp.zeros(left_rim.shape, left_rim.dtype)

    @pl.when(t == end)
    def _():
        right_rim[...] = jnp.zeros(right_rim.shape, right_rim.dtype)

    loads[0].wait()
    rest = phase[...]
    total = jnp.zeros((extent, extent), jnp.float32)
    for _ in range(3):
        part = rest.astype(jnp.bfloat16)
        rest = rest - part.astype(jnp.float32)
        total += exact(exact(sort[...], part).astype(jnp.bfloat16), unsort[...])
    turn[0] = jnp.cos(total)
    sine = jnp.sin(total)
    turn[1] = sine
    turn[2] = -sine
    loads[1].wait()
    loads[2].wait()

    def split(value):
        hi = value.astype(jnp.bfloat16)
        lo = (value - hi.astype(jnp.float32)).astype(jnp.bfloat16)
        return (hi, lo, hi)

    def put_tall(parity, p, value):
        for at, part in enumerate(split(value)):
            talls[parity, pl.ds(at * extent + p * h, h), :] = part

    def put_wide(parity, rows, p, value):
        n = value.shape[0]
        for at, part in enumerate(split(value)):
            wides[parity, pl.ds(rows, n), pl.ds(at * extent + p * h, h)] = part

    def left(at):
        return exact(lefts[at], talls[at % 2])

    def right(at):
        return exact(wides[at % 2], rights[at])

    def halves(load):
        upper, lower = load(slice(0, h)), load(slice(h, extent))
        for p in range(2):
            put_tall(0, p, upper[p] + lower[p])
            put_tall(1, p, upper[p] - lower[p])

    def plain(ref, *at):
        def load(rows):
            return [ref[(*at, p, rows)] for p in range(2)]

        return load

    def through(w, w_at, x, x_at, sign):
        def load(rows):
            wr, wi = w[w_at, 0, rows], w[w_at, 1, rows]
            xr, xi = x[(*x_at, 0, rows)], x[(*x_at, 1, rows)]
            if sign > 0:
                return [wr * xr - wi * xi, wr * xi + wi * xr]
            return [wr * xr + wi * xi, wr * xi - wi * xr]

        return load

    def turned(sine):
        def middle(parity, xr, xi):
            cols = slice(parity * h, (parity + 1) * h)
            kr, ki = turn[0, :, cols], turn[sine, :, cols]
            return kr * xr - ki * xi, kr * xi + ki * xr

        return middle

    def transform(load, middle):
        halves(load)
        for block in range(2):
            half = left(block)
            for p in range(2):
                value = half[p * h : (p + 1) * h]
                put_wide(0, block * h, p, value[:, :h] + value[:, h:])
                put_wide(1, block * h, p, value[:, :h] - value[:, h:])
        for parity in range(2):
            value = right(parity)
            for p, part in enumerate(middle(parity, value[:, :h], value[:, h:])):
                put_wide(parity, 0, p, part)
        u, v = right(2), right(3)
        for p in range(2):
            up, vp = u[:, p * h : (p + 1) * h], v[:, p * h : (p + 1) * h]
            plus, minus = up + vp, up - vp
            for parity in range(2):
                rows = slice(parity * h, (parity + 1) * h)
                put_tall(parity, p, jnp.concatenate([plus[rows], minus[rows]], axis=1))
        u, v = left(2), left(3)
        for p in range(2):
            up, vp = u[p * h : (p + 1) * h], v[p * h : (p + 1) * h]
            spectrum[p, :h] = up + vp
            spectrum[p, h:] = up - vp

    def send_forward(s, part):
        return pltpu.make_async_remote_copy(
            src_ref=leaving.at[s, part], dst_ref=arrived.at[s, part], send_sem=send_f.at[s, part],
            recv_sem=recv_f.at[s, part], device_id={"cuts": g + 1}, device_id_type=MESH)

    def send_backward(s):
        return pltpu.make_async_remote_copy(
            src_ref=adjoint.at[s], dst_ref=backed.at[s], send_sem=send_b.at[s],
            recv_sem=recv_b.at[s], device_id={"cuts": g - 1}, device_id_type=MESH)

    def send_window(s):
        return pltpu.make_async_remote_copy(
            src_ref=windows.at[s], dst_ref=backed.at[s], send_sem=send_b.at[s],
            recv_sem=recv_b.at[s], device_id={"cuts": g - 1}, device_id_type=MESH)

    def far_at(m):
        return slots + m - 1

    def send_own_far():
        return pltpu.make_async_remote_copy(
            src_ref=windows.at[alone], dst_ref=backed.at[far_at(g)], send_sem=send_far.at[g],
            recv_sem=recv_far.at[g], device_id={"cuts": g - 1}, device_id_type=MESH)

    def send_far_on(m):
        return pltpu.make_async_remote_copy(
            src_ref=backed.at[far_at(m)], dst_ref=backed.at[far_at(m)], send_sem=send_far.at[m],
            recv_sem=recv_far.at[m], device_id={"cuts": g - 1}, device_id_type=MESH)

    def compose(s):
        own_part(s).wait()

        @pl.when((t < end) & jnp.logical_not(yielding & (s == turn_of(0))))
        def _():
            rim_copy(0, s).wait_recv()

        @pl.when(t > 0)
        def _():
            rim_copy(1, s).wait_recv()

        for p in range(2):
            windows[s, p, :, :RIM] += left_rim[s, p]
            windows[s, p, :, extent - RIM :] += right_rim[s, p]

    def put_out(j, s):
        src, dst = ((adjoint, adjoint_out), (contrib, contrib_out))[j]
        return pltpu.make_async_copy(src.at[s], dst.at[s], sem_out.at[j, s])

    @pl.when(g == last)
    def _():
        def body(i):
            s = turn_of(i)
            compose(s)

            @pl.when(s == alone)
            def _():
                send_own_far().start()

            @pl.when(s < alone)
            def _():
                send_window(s).start()

        each(body)

    def enter(s):
        @pl.when(g == 0)
        def _():
            arrived[s] = probe[...] * jnp.clip(counts[0] - s, 0, 1).astype(jnp.float32)

        @pl.when(g > 0)
        def _():
            send_forward(s, 0).wait_recv()
            send_forward(s, 1).wait_recv()

        @pl.when((g < last) & ((g == 0) | (s < alone)))
        def _():
            compose(s)

        transform(through(windows, s, arrived, (s,), 1), turned(1))

        @pl.when(g < last)
        def _():
            leaving[s] = spectrum[...]

            @pl.when((g == 0) & ((s > 0) | (t % 2 == 1)))
            def _():
                pl.semaphore_wait(token, 1)

            send_forward(s, 0).start()
            send_forward(s, 1).start()

            @pl.when(g == 0)
            def _():
                send_forward(s, 0).wait_send()

                @pl.when((s < slots - 1) | (t % 2 == 0))
                def _():
                    pl.semaphore_signal(token, inc=1, device_id={"tile": partner}, device_id_type=MESH)

    def beyond(s):
        later = last - g

        @pl.when((g == mid) & (s < alone))
        def _():
            send_window(s).wait_recv()

        @pl.when(g < mid)
        def _():
            spectrum[...] = leaving[s]

        def onward(i, carry):
            spot = jnp.where(s == alone, far_at(g + 1 + i), s)
            transform(through(backed, spot, spectrum, (), 1), turned(1))
            return carry

        lax.fori_loop(0, later, onward, 0)
        seen = exact(sort[...], measured[s]).astype(jnp.bfloat16)
        seen = exact(seen, unsort[...])

        def detected(parity, xr, xi):
            residual = xr * xr + xi * xi - seen[:, parity * h : (parity + 1) * h]
            return xr * residual, xi * residual

        transform(plain(spectrum), detected)
        transform(plain(spectrum), turned(2))

        def homeward(i, carry):
            spot = jnp.where(s == alone, far_at(last - i), s)
            transform(through(backed, spot, spectrum, (), -1), turned(2))
            return carry

        lax.fori_loop(0, later, homeward, 0)

    def back(s):
        send_backward(s).wait_recv()
        transform(plain(backed, s), turned(2))

    def finish_slot(s):
        tr, ti = spectrum[0], spectrum[1]
        wr, wi = windows[s, 0], windows[s, 1]
        adjoint[s, 0] = wr * tr + wi * ti
        adjoint[s, 1] = wr * ti - wi * tr

        @pl.when((g > 0) & (g < last) & (s < alone))
        def _():
            send_backward(s).start()

        xr, xi = arrived[s, 0], arrived[s, 1]
        contrib[s, 0] = xr * tr + xi * ti
        contrib[s, 1] = xr * ti - xi * tr

        @pl.when(t > 0)
        def _():
            got_copy(0, s).start()

        @pl.when(t < end)
        def _():
            got_copy(1, s).start()

        put_out(0, s).start()
        put_out(1, s).start()

    plans = [schedule(here, last, slots) for here in range(sections)]
    width = max(len(plan) for plan in plans)

    def step(e, carry):
        code = jnp.int32(0)
        for here, plan in enumerate(plans):
            for at, (s, act, m) in enumerate(plan):
                code = jnp.where((g == here) & (e == at), (s * 8 + act) * (sections + 1) + m + 1, code)
        m, rest = code % (sections + 1) - 1, code // (sections + 1)
        act, s = rest % 8, rest // 8

        @pl.when((act == ENTER) | (act == WHOLE))
        def _():
            enter(s)

        @pl.when((act == BEYOND) | (act == WHOLE))
        def _():
            beyond(s)

        @pl.when(act == BACK)
        def _():
            back(s)

        @pl.when((act == BEYOND) | (act == WHOLE) | (act == BACK))
        def _():
            finish_slot(s)

        @pl.when(act == OFFER)
        def _():
            compose(alone)
            send_own_far().start()

        @pl.when(act == RELAY)
        def _():
            send_far_on(m).wait_recv()

            @pl.when(g > 0)
            def _():
                send_far_on(m).start()

        return carry

    lax.fori_loop(0, width, step, 0)

    def all_but_lone(action):
        def body(s, carry):
            action(s)
            return carry

        lax.fori_loop(0, alone, body, 0)

    @pl.when(g < last)
    def _():
        each(lambda s: send_forward(s, 1).wait_send())

    @pl.when((g > 0) & (g < last))
    def _():
        each(lambda s: send_forward(s, 0).wait_send())
        all_but_lone(lambda s: send_backward(s).wait_send())

    @pl.when(g == last)
    def _():
        all_but_lone(lambda s: send_window(s).wait_send())

    @pl.when(g > 0)
    def _():
        send_own_far().wait_send()

    for m in range(2, sections):
        @pl.when((g > 0) & (g < m))
        def _():
            send_far_on(m).wait_send()

    @pl.when(t < end)
    def _():
        each(lambda s: got_copy(0, s).wait_recv())

    @pl.when(t > 0)
    def _():
        each(lambda s: got_copy(1, s).wait_recv())

    def finish(side):
        def body(s):
            rim_copy(side, s).wait_send()
            got_copy(side, s).wait_send()

        each(body)

    @pl.when(t > 0)
    def _():
        finish(0)

    @pl.when(t < end)
    def _():
        finish(1)

    each(lambda s: put_out(0, s).wait())
    each(lambda s: put_out(1, s).wait())


def on_device(probe_wave, transmission, kernel_phase, measured, counts, positions, widths):
    f32 = jnp.float32
    bf16 = jnp.bfloat16
    rows, cols = transmission.shape[2:]
    extent = probe_wave.shape[-1]
    slots = positions.shape[1]
    sections = lax.axis_size("cuts")
    tiles = lax.axis_size("tile")
    assert extent == cols and extent >= 2 * RIM and tiles % 2 == 0 and sections >= 2
    own_pos = jnp.concatenate([jnp.swapaxes(positions[0], 0, 1), widths.reshape(2, 1)], 1)
    right_pos = shift(own_pos, "tile", -1)
    left_pos = shift(own_pos, "tile", 1)
    sds = jax.ShapeDtypeStruct
    wave = sds((slots, 2, extent, extent), f32)
    rim = sds((slots, 2, extent, RIM), f32)
    waves = pltpu.VMEM(wave.shape, f32)
    rims = pltpu.VMEM(rim.shape, f32)
    hbm = pl.BlockSpec(memory_space=pl.ANY)
    dma = pltpu.SemaphoreType.DMA
    tall = extent + PAD
    own, to_left, to_right = pl.pallas_call(
        extract_kernel,
        out_shape=(wave, rim, rim),
        in_specs=[smem()] * 3 + [hbm],
        out_specs=(hbm,) * 3,
        scratch_shapes=[
            pltpu.VMEM((slots, 2, tall, RIM), f32),
            pltpu.VMEM((slots, 2, tall, RIM), f32),
            pltpu.VMEM((slots, 2, tall, cols), f32),
            rims, rims, waves,
            dma((3, slots)), dma((3, slots)),
        ],
        compiler_params=params(EXTRACT_VMEM),
    )(left_pos, right_pos, own_pos, transmission[0])
    adjoint, contrib, from_left, from_right = pl.pallas_call(
        functools.partial(pipeline_kernel, sections, tiles),
        out_shape=(wave, wave, rim, rim),
        in_specs=[smem()] + [hbm] * 6 + [vmem()] * 10,
        out_specs=(hbm,) * 4,
        scratch_shapes=[
            pltpu.VMEM((2, extent, extent), f32),
            pltpu.VMEM((extent, extent), f32),
            pltpu.VMEM((slots, extent, extent), bf16),
            waves, rims, rims,
            waves, waves,
            pltpu.VMEM((slots + sections - 1, 2, extent, extent), f32),
            waves, waves,
            pltpu.VMEM((4, extent, 3 * extent), bf16),
            pltpu.VMEM((4, 3 * extent, extent), bf16),
            pltpu.VMEM((3, extent, extent), f32),
            pltpu.VMEM((2, 3 * extent, extent), bf16),
            pltpu.VMEM((2, extent, 3 * extent), bf16),
            pltpu.VMEM((2, extent, extent), f32),
            dma((3,)),
            dma((slots,)),
            dma((2, slots)),
            dma((slots, 2)), dma((slots, 2)),
            dma((slots,)), dma((slots,)),
            dma((sections,)), dma((sections,)),
            dma((2, slots)), dma((2, slots)),
            dma((2, slots)), dma((2, slots)),
            pltpu.SemaphoreType.REGULAR,
        ],
        compiler_params=params(PIPELINE_VMEM, collective_id=0, has_side_effects=True),
    )(counts, own, to_left, to_right, probe_wave, kernel_phase, measured[0], *make_tables(extent))
    grad, entry = pl.pallas_call(
        gather_kernel,
        out_shape=(sds((2, rows, cols), f32), wave),
        in_specs=[smem()] * 3 + [hbm] * 4,
        out_specs=(hbm, hbm),
        scratch_shapes=[
            pltpu.VMEM((2, rows, cols), f32), waves, rims, rims, waves,
            dma((3, slots)), dma((2,)), dma((2,)),
        ],
        compiler_params=params(GATHER_VMEM),
    )(left_pos, right_pos, own_pos, contrib, from_left, from_right, adjoint)
    return (entry[None, None], grad[None])


def solution(mesh):
    return jax.shard_map(
        on_device,
        mesh=mesh,
        in_specs=(
            P(),
            P("cuts", None, None, "tile"),
            P(),
            P("tile", None, None, None),
            P("tile"),
            P("tile", None, None),
            P("tile", None),
        ),
        out_specs=(P("cuts", "tile", None, None, None, None), P("cuts", None, None, "tile")),
        check_vma=False,
    )
```

```python
import functools
import math

import jax
import jax.numpy as jnp
import numpy as np
from jax import lax
from jax.experimental import pallas as pl
from jax.experimental.pallas import tpu as pltpu
from jax.sharding import PartitionSpec as P

RIM = 128
PAD = 8
MESH = pl.DeviceIdType.MESH
MIB = 1024 * 1024
EXTRACT_VMEM = 62 * MIB
PIPELINE_VMEM = 62 * MIB
GATHER_VMEM = 62 * MIB


def params(limit, **kw):
    return pltpu.CompilerParams(vmem_limit_bytes=limit, **kw)


def vmem():
    return pl.BlockSpec(memory_space=pltpu.VMEM)


def smem():
    return pl.BlockSpec(memory_space=pltpu.SMEM)


def make_tables(extent):
    half = extent // 2
    indices = np.arange(extent)
    angles = (indices[:, None] * indices[None, :] % extent) * (2.0 * math.pi / extent)
    cosine = (np.cos(angles) / math.sqrt(extent)).astype(np.float32)
    sine = (np.sin(angles) / math.sqrt(extent)).astype(np.float32)
    tables = []
    for parity in range(2):
        c, s = cosine[parity::2, :half], sine[parity::2, :half]
        block = np.block([[c, s], [-s, c]])
        for matrix in (block, block.T):
            hi = matrix.astype(jnp.bfloat16)
            lo = (matrix - hi.astype(np.float32)).astype(jnp.bfloat16)
            tables += [jnp.asarray(hi), jnp.asarray(lo)]
    order = np.concatenate([indices[0::2], indices[1::2]])
    sort = (order[:, None] == indices[None, :]).astype(jnp.bfloat16)
    return tables + [jnp.asarray(sort), jnp.asarray(np.ascontiguousarray(sort.T))]


def aligned(row, limit):
    base = jnp.minimum(row // PAD * PAD, limit)
    return pl.multiple_of(base, PAD), row - base


def exchange_kernel(tiles, places, widths, left, right, own, box_places, box_widths, send, recv):
    t = lax.axis_index("tile")
    slots = places.shape[1]
    barrier = pltpu.get_barrier_semaphore()
    inside = (t > 0, t < tiles - 1)
    for side in range(2):
        @pl.when(inside[side])
        def _():
            pl.semaphore_signal(
                barrier, inc=1, device_id={"tile": t + (-1, 1)[side]}, device_id_type=MESH)

    def copies(side):
        return [
            pltpu.make_async_remote_copy(
                src_ref=src, dst_ref=dst.at[side], send_sem=send.at[i, side],
                recv_sem=recv.at[i, side], device_id={"tile": t + (-1, 1)[side]},
                device_id_type=MESH)
            for i, (src, dst) in enumerate(((places, box_places), (widths, box_widths)))
        ]

    pl.semaphore_wait(barrier, inside[0].astype(jnp.int32) + inside[1].astype(jnp.int32))
    for side in range(2):
        @pl.when(inside[side])
        def _():
            for copy in copies(side):
                copy.start()

    for k in range(2):
        for s in range(slots):
            own[k, s] = places[k, s]
        own[k, slots] = widths[0, k]

    for side, out in enumerate((left, right)):
        @pl.when(inside[side])
        def _():
            for copy in copies(1 - side):
                copy.wait_recv()
            for k in range(2):
                for s in range(slots):
                    out[k, s] = box_places[1 - side, k, s]
                out[k, slots] = box_widths[1 - side, 0, k]
            for copy in copies(side):
                copy.wait_send()

        @pl.when(jnp.logical_not(inside[side]))
        def _():
            for k in range(2):
                for s in range(slots + 1):
                    out[k, s] = 0


def extract_kernel(left_pos, right_pos, own_pos, trans, own, to_left, to_right,
                   buf_left, buf_right, buf_own, out_left, out_right, out_own, sem_in, sem_out):
    t = lax.axis_index("tile")
    end = lax.axis_size("tile") - 1
    slots, _, extent, _ = own.shape
    rows, cols = trans.shape[1:]
    tall = extent + PAD
    slack = cols + 2 * RIM - extent
    jobs = (
        (left_pos, buf_left, 0, RIM, out_left, to_left),
        (right_pos, buf_right, cols - RIM, RIM, out_right, to_right),
        (own_pos, buf_own, 0, cols, out_own, own),
    )

    def fetch(j, s):
        pos, buf, start, width = jobs[j][:4]
        base, off = aligned(pos[0, s], rows - tall)
        src = trans.at[:, pl.ds(base, tall), pl.ds(start, width)]
        return pltpu.make_async_copy(src, buf.at[s], sem_in.at[j, s]), off

    def flush(j, s):
        return pltpu.make_async_copy(jobs[j][4].at[s], jobs[j][5].at[s], sem_out.at[j, s])

    for s in range(slots):
        for j in range(3):
            fetch(j, s)[0].start()

    def columns(width):
        return lax.broadcasted_iota(jnp.int32, (extent, width), 1)

    def load(j, s, p, off, turn):
        value = pltpu.roll(jobs[j][1][s, p], (tall - off) % tall, 0)[:extent]
        return pltpu.roll(value, turn, 1)

    def body(s, carry):
        one, off = fetch(0, s)
        one.wait()
        short = slack - left_pos[1, s]
        at = columns(RIM) - short
        good = (at >= 0) & (at + 1 <= left_pos[1, slots])
        for p in range(2):
            out_left[s, p] = jnp.where(good, load(0, s, p, off, short % RIM), 0.0)
        flush(0, s).start()
        one, off = fetch(1, s)
        one.wait()
        col = right_pos[1, s]
        at = columns(RIM) + col
        good = (at < RIM) & (RIM - at <= right_pos[0, slots])
        for p in range(2):
            out_right[s, p] = jnp.where(good, load(1, s, p, off, (cols - col) % RIM), 0.0)
        flush(1, s).start()
        one, off = fetch(2, s)
        one.wait()
        col = own_pos[1, s]
        at = columns(extent) + col
        middle = (at >= RIM) & (at < RIM + cols)
        left_ok = (t > 0) & (at < RIM) & (RIM - at <= own_pos[0, slots])
        right_ok = (t < end) & (at >= RIM + cols) & (at - RIM - cols + 1 <= own_pos[1, slots])
        rim = left_ok | right_ok
        for p in range(2):
            value = load(2, s, p, off, (cols + RIM - col) % cols)
            out_own[s, p] = jnp.where(middle, value, jnp.where(rim, 0.0, 1.0 - p))
        flush(2, s).start()
        return carry

    lax.fori_loop(0, slots, body, 0)
    for s in range(slots):
        for j in range(3):
            flush(j, s).wait()


def gather_kernel(left_pos, right_pos, own_pos, contrib, from_left,
                  from_right, adjoint, grad, entry, acc, buf_own, buf_left, buf_right, buf_entry,
                  sem_in, sem_entry, sem_grad):
    slots, _, extent, _ = buf_own.shape
    rows, cols = acc.shape[1:]
    tall = extent + PAD
    slack = cols + 2 * RIM - extent
    jobs = ((contrib, buf_own), (from_left, buf_left), (from_right, buf_right))

    def fetch(j, s):
        return pltpu.make_async_copy(jobs[j][0].at[s], jobs[j][1].at[s], sem_in.at[j, s])

    for s in range(slots):
        for j in range(3):
            fetch(j, s).start()
    entry_in = pltpu.make_async_copy(adjoint, buf_entry, sem_entry.at[0])
    entry_out = pltpu.make_async_copy(buf_entry, entry, sem_entry.at[1])
    entry_in.start()
    acc[...] = jnp.zeros(acc.shape, acc.dtype)

    def columns(width):
        return lax.broadcasted_iota(jnp.int32, (extent, width), 1)

    def add(source, s, p, row, good, turn, start, width):
        base, off = aligned(row, rows - tall)
        value = jnp.where(good, pltpu.roll(source[s, p], turn, 1), 0.0)
        value = jnp.concatenate([value, jnp.zeros((PAD, width), jnp.float32)], axis=0)
        acc[p, pl.ds(base, tall), pl.ds(start, width)] += pltpu.roll(value, off, 0)

    def plane(p):
        def body(s, carry):
            if p == 0:
                for j in range(3):
                    fetch(j, s).wait()
            col = own_pos[1, s]
            at = columns(cols) + RIM - col
            good = (at >= 0) & (at < extent)
            add(buf_own, s, p, own_pos[0, s], good, (col + cols - RIM) % cols, 0, cols)
            short = slack - left_pos[1, s]
            at = columns(RIM)
            good = (at + short < RIM) & (at + 1 <= left_pos[1, slots])
            add(buf_left, s, p, left_pos[0, s], good, (cols - short) % RIM, 0, RIM)
            col = right_pos[1, s]
            good = (at >= col) & (RIM - at <= right_pos[0, slots])
            add(buf_right, s, p, right_pos[0, s], good, col % RIM, cols - RIM, RIM)
            return carry

        lax.fori_loop(0, slots, body, 0)

    def flush(p):
        return pltpu.make_async_copy(acc.at[p], grad.at[p], sem_grad.at[p])

    plane(0)
    flush(0).start()
    entry_in.wait()
    entry_out.start()
    plane(1)
    flush(1).start()
    entry_out.wait()
    flush(0).wait()
    flush(1).wait()


ENTER, BEYOND, WHOLE, BACK, OFFER, RELAY = range(1, 7)


def schedule(g, last, slots):
    mid, alone = last - 1, slots - 1
    relays = [(0, RELAY, m) for m in range(g + 1, last + 1)]
    plan = [(0, OFFER, g)] * (0 < g < last)
    if g >= mid:
        return plan + relays + [(s, WHOLE, g) for s in range(slots)]
    lag = 2 * (mid - g)
    done = 0
    for k in range(slots):
        plan += [(k, ENTER, g)]
        if g > 0 and relays:
            plan += [relays.pop(0)]
        if k >= lag:
            plan += [(done, BACK, g)]
            done += 1
    while done < alone - 2:
        plan += [(done, BACK, g)]
        done += 1
    plan += relays + [(alone, BEYOND, g)]
    while done < alone:
        plan += [(done, BACK, g)]
        done += 1
    return plan


def pipeline_kernel(sections, tiles, counts, own, to_left, to_right, hbm_probe, hbm_phase, hbm_measured,
                    ef_hi, ef_lo, ei_hi, ei_lo, of_hi, of_lo, oi_hi, oi_lo, sort, unsort,
                    adjoint_out, contrib_out, from_left, from_right,
                    probe, phase, measured,
                    windows, left_rim, right_rim, arrived, leaving, backed, adjoint, contrib,
                    lefts, rights, turn, talls, wides, spectrum,
                    sem_in, sem_own, sem_out, send_f, recv_f, send_b, recv_b, send_far, recv_far,
                    send_rim, recv_rim, send_got, recv_got, token):
    g = lax.axis_index("cuts")
    t = lax.axis_index("tile")
    last = sections - 1
    mid = last - 1
    end = tiles - 1
    slots, _, extent, _ = windows.shape
    h = extent // 2
    partner = t + 1 - 2 * (t % 2)
    alone = slots - 1

    loads = [
        pltpu.make_async_copy(src, dst, sem_in.at[i])
        for i, (src, dst) in enumerate(
            ((hbm_phase, phase), (hbm_probe, probe), (hbm_measured, measured)))
    ]

    def own_part(s):
        return pltpu.make_async_copy(own.at[s], windows.at[s], sem_own.at[s])

    barrier = pltpu.get_barrier_semaphore()

    @pl.when(g > 0)
    def _():
        pl.semaphore_signal(barrier, inc=1, device_id={"cuts": g - 1}, device_id_type=MESH)

    @pl.when(g < last)
    def _():
        pl.semaphore_signal(barrier, inc=1, device_id={"cuts": g + 1}, device_id_type=MESH)

    @pl.when(t > 0)
    def _():
        pl.semaphore_signal(barrier, inc=1, device_id={"tile": t - 1}, device_id_type=MESH)

    @pl.when(t < end)
    def _():
        pl.semaphore_signal(barrier, inc=1, device_id={"tile": t + 1}, device_id_type=MESH)

    def exact(x, y):
        return jnp.dot(x, y, preferred_element_type=jnp.float32)

    def each(action):
        def body(s, carry):
            action(s)
            return carry

        lax.fori_loop(0, slots, body, 0)

    for load in loads:
        load.start()
    each(lambda s: own_part(s).start())

    def turn_of(i):
        return (i + alone * ((g + last - 1) // last)) % slots

    forms = ((ef_hi, ef_lo, ei_hi, ei_lo), (of_hi, of_lo, oi_hi, oi_lo))
    for parity in range(2):
        fh, fl, ih, il = forms[parity]
        for inverse, (lh, ll, rh, rl) in enumerate(((fh, fl, ih, il), (ih, il, fh, fl))):
            at = 2 * inverse + parity
            lefts[at, :, :extent] = lh[...]
            lefts[at, :, extent : 2 * extent] = lh[...]
            lefts[at, :, 2 * extent :] = ll[...]
            rights[at, :extent] = rh[...]
            rights[at, extent : 2 * extent] = rh[...]
            rights[at, 2 * extent :] = rl[...]

    peers = (g + last - 1) // last + 1 - g // last + (t + end - 1) // end + 1 - t // end
    pl.semaphore_wait(barrier, peers)

    def rim_copy(side, s):
        src, dst = ((to_left, right_rim), (to_right, left_rim))[side]
        return pltpu.make_async_remote_copy(
            src_ref=src.at[s], dst_ref=dst.at[s], send_sem=send_rim.at[side, s],
            recv_sem=recv_rim.at[side, s], device_id={"tile": t + (-1, 1)[side]},
            device_id_type=MESH)

    def got_copy(side, s):
        start, dst = ((0, from_right), (extent - RIM, from_left))[side]
        return pltpu.make_async_remote_copy(
            src_ref=contrib.at[s, :, :, pl.ds(start, RIM)], dst_ref=dst.at[s],
            send_sem=send_got.at[side, s], recv_sem=recv_got.at[side, s],
            device_id={"tile": t + (-1, 1)[side]}, device_id_type=MESH)

    yielding = (t % 2 == 0) & (t > 0)

    def rims_start(side, s, ok):
        @pl.when(ok)
        def _():
            rim_copy(side, s).start()

    def rims_one(i):
        s = turn_of(i)
        rims_start(0, s, (t > 0) & jnp.logical_not(yielding))
        rims_start(1, s, t < end)

    each(rims_one)

    @pl.when(yielding)
    def _():
        rim_copy(0, turn_of(0)).wait_recv()

    each(lambda i: rims_start(0, turn_of(i), yielding))

    @pl.when(t == 0)
    def _():
        left_rim[...] = jnp.zeros(left_rim.shape, left_rim.dtype)

    @pl.when(t == end)
    def _():
        right_rim[...] = jnp.zeros(right_rim.shape, right_rim.dtype)

    loads[0].wait()
    rest = phase[...]
    total = jnp.zeros((extent, extent), jnp.float32)
    for _ in range(3):
        part = rest.astype(jnp.bfloat16)
        rest = rest - part.astype(jnp.float32)
        total += exact(exact(sort[...], part).astype(jnp.bfloat16), unsort[...])
    turn[0] = jnp.cos(total)
    sine = jnp.sin(total)
    turn[1] = sine
    turn[2] = -sine
    loads[1].wait()
    loads[2].wait()

    def split(value):
        hi = value.astype(jnp.bfloat16)
        lo = (value - hi.astype(jnp.float32)).astype(jnp.bfloat16)
        return (hi, lo, hi)

    def put_tall(parity, p, value):
        for at, part in enumerate(split(value)):
            talls[parity, pl.ds(at * extent + p * h, h), :] = part

    def put_wide(parity, rows, p, value):
        n = value.shape[0]
        for at, part in enumerate(split(value)):
            wides[parity, pl.ds(rows, n), pl.ds(at * extent + p * h, h)] = part

    def left(at):
        return exact(lefts[at], talls[at % 2])

    def right(at):
        return exact(wides[at % 2], rights[at])

    def halves(load):
        upper, lower = load(slice(0, h)), load(slice(h, extent))
        for p in range(2):
            put_tall(0, p, upper[p] + lower[p])
            put_tall(1, p, upper[p] - lower[p])

    def plain(ref, *at):
        def load(rows):
            return [ref[(*at, p, rows)] for p in range(2)]

        return load

    def through(w, w_at, x, x_at, sign):
        def load(rows):
            wr, wi = w[w_at, 0, rows], w[w_at, 1, rows]
            xr, xi = x[(*x_at, 0, rows)], x[(*x_at, 1, rows)]
            if sign > 0:
                return [wr * xr - wi * xi, wr * xi + wi * xr]
            return [wr * xr + wi * xi, wr * xi - wi * xr]

        return load

    def turned(sine):
        def middle(parity, xr, xi):
            cols = slice(parity * h, (parity + 1) * h)
            kr, ki = turn[0, :, cols], turn[sine, :, cols]
            return kr * xr - ki * xi, kr * xi + ki * xr

        return middle

    def transform(load, middle):
        halves(load)
        for block in range(2):
            half = left(block)
            for p in range(2):
                value = half[p * h : (p + 1) * h]
                put_wide(0, block * h, p, value[:, :h] + value[:, h:])
                put_wide(1, block * h, p, value[:, :h] - value[:, h:])
        for parity in range(2):
            value = right(parity)
            for p, part in enumerate(middle(parity, value[:, :h], value[:, h:])):
                put_wide(parity, 0, p, part)
        u, v = right(2), right(3)
        for p in range(2):
            up, vp = u[:, p * h : (p + 1) * h], v[:, p * h : (p + 1) * h]
            plus, minus = up + vp, up - vp
            for parity in range(2):
                rows = slice(parity * h, (parity + 1) * h)
                put_tall(parity, p, jnp.concatenate([plus[rows], minus[rows]], axis=1))
        u, v = left(2), left(3)
        for p in range(2):
            up, vp = u[p * h : (p + 1) * h], v[p * h : (p + 1) * h]
            spectrum[p, :h] = up + vp
            spectrum[p, h:] = up - vp

    def send_forward(s, part):
        return pltpu.make_async_remote_copy(
            src_ref=leaving.at[s, part], dst_ref=arrived.at[s, part], send_sem=send_f.at[s, part],
            recv_sem=recv_f.at[s, part], device_id={"cuts": g + 1}, device_id_type=MESH)

    def send_backward(s):
        return pltpu.make_async_remote_copy(
            src_ref=adjoint.at[s], dst_ref=backed.at[s], send_sem=send_b.at[s],
            recv_sem=recv_b.at[s], device_id={"cuts": g - 1}, device_id_type=MESH)

    def send_window(s):
        return pltpu.make_async_remote_copy(
            src_ref=windows.at[s], dst_ref=backed.at[s], send_sem=send_b.at[s],
            recv_sem=recv_b.at[s], device_id={"cuts": g - 1}, device_id_type=MESH)

    def far_at(m):
        return slots + m - 1

    def send_own_far():
        return pltpu.make_async_remote_copy(
            src_ref=windows.at[alone], dst_ref=backed.at[far_at(g)], send_sem=send_far.at[g],
            recv_sem=recv_far.at[g], device_id={"cuts": g - 1}, device_id_type=MESH)

    def send_far_on(m):
        return pltpu.make_async_remote_copy(
            src_ref=backed.at[far_at(m)], dst_ref=backed.at[far_at(m)], send_sem=send_far.at[m],
            recv_sem=recv_far.at[m], device_id={"cuts": g - 1}, device_id_type=MESH)

    def compose(s):
        own_part(s).wait()

        @pl.when((t < end) & jnp.logical_not(yielding & (s == turn_of(0))))
        def _():
            rim_copy(0, s).wait_recv()

        @pl.when(t > 0)
        def _():
            rim_copy(1, s).wait_recv()

        for p in range(2):
            windows[s, p, :, :RIM] += left_rim[s, p]
            windows[s, p, :, extent - RIM :] += right_rim[s, p]

    def put_out(j, s):
        src, dst = ((adjoint, adjoint_out), (contrib, contrib_out))[j]
        return pltpu.make_async_copy(src.at[s], dst.at[s], sem_out.at[j, s])

    @pl.when(g == last)
    def _():
        def body(i):
            s = turn_of(i)
            compose(s)

            @pl.when(s == alone)
            def _():
                send_own_far().start()

            @pl.when(s < alone)
            def _():
                send_window(s).start()

        each(body)

    def enter(s):
        @pl.when(g == 0)
        def _():
            arrived[s] = probe[...] * jnp.clip(counts[0] - s, 0, 1).astype(jnp.float32)

        @pl.when(g > 0)
        def _():
            send_forward(s, 0).wait_recv()
            send_forward(s, 1).wait_recv()

        @pl.when((g < last) & ((g == 0) | (s < alone)))
        def _():
            compose(s)

        transform(through(windows, s, arrived, (s,), 1), turned(1))

        @pl.when(g < last)
        def _():
            leaving[s] = spectrum[...]

            @pl.when((g == 0) & ((s > 0) | (t % 2 == 1)))
            def _():
                pl.semaphore_wait(token, 1)

            send_forward(s, 0).start()
            send_forward(s, 1).start()

            @pl.when(g == 0)
            def _():
                send_forward(s, 0).wait_send()

                @pl.when((s < slots - 1) | (t % 2 == 0))
                def _():
                    pl.semaphore_signal(token, inc=1, device_id={"tile": partner}, device_id_type=MESH)

    def beyond(s):
        later = last - g

        @pl.when((g == mid) & (s < alone))
        def _():
            send_window(s).wait_recv()

        @pl.when(g < mid)
        def _():
            spectrum[...] = leaving[s]

        def onward(i, carry):
            spot = jnp.where(s == alone, far_at(g + 1 + i), s)
            transform(through(backed, spot, spectrum, (), 1), turned(1))
            return carry

        lax.fori_loop(0, later, onward, 0)
        seen = exact(sort[...], measured[s]).astype(jnp.bfloat16)
        seen = exact(seen, unsort[...])

        def detected(parity, xr, xi):
            residual = xr * xr + xi * xi - seen[:, parity * h : (parity + 1) * h]
            return xr * residual, xi * residual

        transform(plain(spectrum), detected)
        transform(plain(spectrum), turned(2))

        def homeward(i, carry):
            spot = jnp.where(s == alone, far_at(last - i), s)
            transform(through(backed, spot, spectrum, (), -1), turned(2))
            return carry

        lax.fori_loop(0, later, homeward, 0)

    def back(s):
        send_backward(s).wait_recv()
        transform(plain(backed, s), turned(2))

    def finish_slot(s):
        tr, ti = spectrum[0], spectrum[1]
        wr, wi = windows[s, 0], windows[s, 1]
        adjoint[s, 0] = wr * tr + wi * ti
        adjoint[s, 1] = wr * ti - wi * tr

        @pl.when((g > 0) & (g < last) & (s < alone))
        def _():
            send_backward(s).start()

        xr, xi = arrived[s, 0], arrived[s, 1]
        contrib[s, 0] = xr * tr + xi * ti
        contrib[s, 1] = xr * ti - xi * tr

        @pl.when(t > 0)
        def _():
            got_copy(0, s).start()

        @pl.when(t < end)
        def _():
            got_copy(1, s).start()

        put_out(0, s).start()
        put_out(1, s).start()

    plans = [schedule(here, last, slots) for here in range(sections)]
    width = max(len(plan) for plan in plans)

    def step(e, carry):
        code = jnp.int32(0)
        for here, plan in enumerate(plans):
            for at, (s, act, m) in enumerate(plan):
                code = jnp.where((g == here) & (e == at), (s * 8 + act) * (sections + 1) + m + 1, code)
        m, rest = code % (sections + 1) - 1, code // (sections + 1)
        act, s = rest % 8, rest // 8

        @pl.when((act == ENTER) | (act == WHOLE))
        def _():
            enter(s)

        @pl.when((act == BEYOND) | (act == WHOLE))
        def _():
            beyond(s)

        @pl.when(act == BACK)
        def _():
            back(s)

        @pl.when((act == BEYOND) | (act == WHOLE) | (act == BACK))
        def _():
            finish_slot(s)

        @pl.when(act == OFFER)
        def _():
            compose(alone)
            send_own_far().start()

        @pl.when(act == RELAY)
        def _():
            send_far_on(m).wait_recv()

            @pl.when(g > 0)
            def _():
                send_far_on(m).start()

        return carry

    lax.fori_loop(0, width, step, 0)

    def all_but_lone(action):
        def body(s, carry):
            action(s)
            return carry

        lax.fori_loop(0, alone, body, 0)

    @pl.when(g < last)
    def _():
        each(lambda s: send_forward(s, 1).wait_send())

    @pl.when((g > 0) & (g < last))
    def _():
        each(lambda s: send_forward(s, 0).wait_send())
        all_but_lone(lambda s: send_backward(s).wait_send())

    @pl.when(g == last)
    def _():
        all_but_lone(lambda s: send_window(s).wait_send())

    @pl.when(g > 0)
    def _():
        send_own_far().wait_send()

    for m in range(2, sections):
        @pl.when((g > 0) & (g < m))
        def _():
            send_far_on(m).wait_send()

    @pl.when(t < end)
    def _():
        each(lambda s: got_copy(0, s).wait_recv())

    @pl.when(t > 0)
    def _():
        each(lambda s: got_copy(1, s).wait_recv())

    def finish(side):
        def body(s):
            rim_copy(side, s).wait_send()
            got_copy(side, s).wait_send()

        each(body)

    @pl.when(t > 0)
    def _():
        finish(0)

    @pl.when(t < end)
    def _():
        finish(1)

    each(lambda s: put_out(0, s).wait())
    each(lambda s: put_out(1, s).wait())


def on_device(probe_wave, transmission, kernel_phase, measured, counts, positions, widths):
    f32 = jnp.float32
    bf16 = jnp.bfloat16
    rows, cols = transmission.shape[2:]
    extent = probe_wave.shape[-1]
    slots = positions.shape[1]
    sections = lax.axis_size("cuts")
    tiles = lax.axis_size("tile")
    assert extent == cols and extent >= 2 * RIM and tiles % 2 == 0 and sections >= 2
    sds = jax.ShapeDtypeStruct
    wave = sds((slots, 2, extent, extent), f32)
    rim = sds((slots, 2, extent, RIM), f32)
    waves = pltpu.VMEM(wave.shape, f32)
    rims = pltpu.VMEM(rim.shape, f32)
    hbm = pl.BlockSpec(memory_space=pl.ANY)
    dma = pltpu.SemaphoreType.DMA
    tall = extent + PAD
    marks = sds((2, slots + 1), jnp.int32)
    left_pos, right_pos, own_pos = pl.pallas_call(
        functools.partial(exchange_kernel, tiles),
        out_shape=(marks,) * 3,
        in_specs=[smem()] * 2,
        out_specs=(smem(),) * 3,
        scratch_shapes=[
            pltpu.SMEM((2, 2, slots), jnp.int32),
            pltpu.SMEM((2, 1, 2), jnp.int32),
            dma((2, 2)), dma((2, 2)),
        ],
        compiler_params=params(EXTRACT_VMEM, collective_id=1, has_side_effects=True),
    )(jnp.swapaxes(positions[0], 0, 1), widths)
    own, to_left, to_right = pl.pallas_call(
        extract_kernel,
        out_shape=(wave, rim, rim),
        in_specs=[smem()] * 3 + [hbm],
        out_specs=(hbm,) * 3,
        scratch_shapes=[
            pltpu.VMEM((slots, 2, tall, RIM), f32),
            pltpu.VMEM((slots, 2, tall, RIM), f32),
            pltpu.VMEM((slots, 2, tall, cols), f32),
            rims, rims, waves,
            dma((3, slots)), dma((3, slots)),
        ],
        compiler_params=params(EXTRACT_VMEM),
    )(left_pos, right_pos, own_pos, transmission[0])
    adjoint, contrib, from_left, from_right = pl.pallas_call(
        functools.partial(pipeline_kernel, sections, tiles),
        out_shape=(wave, wave, rim, rim),
        in_specs=[smem()] + [hbm] * 6 + [vmem()] * 10,
        out_specs=(hbm,) * 4,
        scratch_shapes=[
            pltpu.VMEM((2, extent, extent), f32),
            pltpu.VMEM((extent, extent), f32),
            pltpu.VMEM((slots, extent, extent), bf16),
            waves, rims, rims,
            waves, waves,
            pltpu.VMEM((slots + sections - 1, 2, extent, extent), f32),
            waves, waves,
            pltpu.VMEM((4, extent, 3 * extent), bf16),
            pltpu.VMEM((4, 3 * extent, extent), bf16),
            pltpu.VMEM((3, extent, extent), f32),
            pltpu.VMEM((2, 3 * extent, extent), bf16),
            pltpu.VMEM((2, extent, 3 * extent), bf16),
            pltpu.VMEM((2, extent, extent), f32),
            dma((3,)),
            dma((slots,)),
            dma((2, slots)),
            dma((slots, 2)), dma((slots, 2)),
            dma((slots,)), dma((slots,)),
            dma((sections,)), dma((sections,)),
            dma((2, slots)), dma((2, slots)),
            dma((2, slots)), dma((2, slots)),
            pltpu.SemaphoreType.REGULAR,
        ],
        compiler_params=params(PIPELINE_VMEM, collective_id=0, has_side_effects=True),
    )(counts, own, to_left, to_right, probe_wave, kernel_phase, measured[0], *make_tables(extent))
    grad, entry = pl.pallas_call(
        gather_kernel,
        out_shape=(sds((2, rows, cols), f32), wave),
        in_specs=[smem()] * 3 + [hbm] * 4,
        out_specs=(hbm, hbm),
        scratch_shapes=[
            pltpu.VMEM((2, rows, cols), f32), waves, rims, rims, waves,
            dma((3, slots)), dma((2,)), dma((2,)),
        ],
        compiler_params=params(GATHER_VMEM),
    )(left_pos, right_pos, own_pos, contrib, from_left, from_right, adjoint)
    return (entry[None, None], grad[None])


def solution(mesh):
    return jax.shard_map(
        on_device,
        mesh=mesh,
        in_specs=(
            P(),
            P("cuts", None, None, "tile"),
            P(),
            P("tile", None, None, None),
            P("tile"),
            P("tile", None, None),
            P("tile", None),
        ),
        out_specs=(P("cuts", "tile", None, None, None, None), P("cuts", None, None, "tile")),
        check_vma=False,
    )
```

```python
import functools
import math

import jax
import jax.numpy as jnp
import numpy as np
from jax import lax
from jax.experimental import pallas as pl
from jax.experimental.pallas import tpu as pltpu
from jax.sharding import PartitionSpec as P

RIM = 128
PAD = 8
MESH = pl.DeviceIdType.MESH
MIB = 1024 * 1024
EXTRACT_VMEM = 62 * MIB
PIPELINE_VMEM = 62 * MIB
GATHER_VMEM = 62 * MIB


def params(limit, **kw):
    return pltpu.CompilerParams(vmem_limit_bytes=limit, **kw)


def vmem():
    return pl.BlockSpec(memory_space=pltpu.VMEM)


def smem():
    return pl.BlockSpec(memory_space=pltpu.SMEM)


def make_tables(extent):
    half = extent // 2
    indices = np.arange(extent)
    angles = (indices[:, None] * indices[None, :] % extent) * (2.0 * math.pi / extent)
    cosine = (np.cos(angles) / math.sqrt(extent)).astype(np.float32)
    sine = (np.sin(angles) / math.sqrt(extent)).astype(np.float32)
    tables = []
    for parity in range(2):
        c, s = cosine[parity::2, :half], sine[parity::2, :half]
        block = np.block([[c, s], [-s, c]])
        for matrix in (block, block.T):
            hi = matrix.astype(jnp.bfloat16)
            lo = (matrix - hi.astype(np.float32)).astype(jnp.bfloat16)
            tables += [jnp.asarray(hi), jnp.asarray(lo)]
    order = np.concatenate([indices[0::2], indices[1::2]])
    sort = (order[:, None] == indices[None, :]).astype(jnp.bfloat16)
    return tables + [jnp.asarray(sort), jnp.asarray(np.ascontiguousarray(sort.T))]


def aligned(row, limit):
    base = jnp.minimum(row // PAD * PAD, limit)
    return pl.multiple_of(base, PAD), row - base


def exchange_kernel(tiles, places, widths, left, right, own, box_places, box_widths, send, recv):
    t = lax.axis_index("tile")
    slots = places.shape[1]
    barrier = pltpu.get_barrier_semaphore()
    inside = (t > 0, t < tiles - 1)
    for side in range(2):
        @pl.when(inside[side])
        def _():
            pl.semaphore_signal(
                barrier, inc=1, device_id={"tile": t + (-1, 1)[side]}, device_id_type=MESH)

    def copies(side):
        return [
            pltpu.make_async_remote_copy(
                src_ref=src, dst_ref=dst.at[side], send_sem=send.at[i, side],
                recv_sem=recv.at[i, side], device_id={"tile": t + (-1, 1)[side]},
                device_id_type=MESH)
            for i, (src, dst) in enumerate(((places, box_places), (widths, box_widths)))
        ]

    pl.semaphore_wait(barrier, inside[0].astype(jnp.int32) + inside[1].astype(jnp.int32))
    for side in range(2):
        @pl.when(inside[side])
        def _():
            for copy in copies(side):
                copy.start()

    for k in range(2):
        for s in range(slots):
            own[k, s] = places[k, s]
        own[k, slots] = widths[0, k]

    for side, out in enumerate((left, right)):
        @pl.when(inside[side])
        def _():
            for copy in copies(1 - side):
                copy.wait_recv()
            for k in range(2):
                for s in range(slots):
                    out[k, s] = box_places[1 - side, k, s]
                out[k, slots] = box_widths[1 - side, 0, k]
            for copy in copies(side):
                copy.wait_send()

        @pl.when(jnp.logical_not(inside[side]))
        def _():
            for k in range(2):
                for s in range(slots + 1):
                    out[k, s] = 0


def extract_kernel(left_pos, right_pos, own_pos, trans, own, to_left, to_right,
                   buf_left, buf_right, buf_own, out_left, out_right, out_own, sem_in, sem_out):
    t = lax.axis_index("tile")
    end = lax.axis_size("tile") - 1
    slots, _, extent, _ = own.shape
    rows, cols = trans.shape[1:]
    tall = extent + PAD
    slack = cols + 2 * RIM - extent
    jobs = (
        (left_pos, buf_left, 0, RIM, out_left, to_left),
        (right_pos, buf_right, cols - RIM, RIM, out_right, to_right),
        (own_pos, buf_own, 0, cols, out_own, own),
    )

    def fetch(j, s):
        pos, buf, start, width = jobs[j][:4]
        base, off = aligned(pos[0, s], rows - tall)
        src = trans.at[:, pl.ds(base, tall), pl.ds(start, width)]
        return pltpu.make_async_copy(src, buf.at[s], sem_in.at[j, s]), off

    def flush(j, s):
        return pltpu.make_async_copy(jobs[j][4].at[s], jobs[j][5].at[s], sem_out.at[j, s])

    for s in range(slots):
        for j in range(3):
            fetch(j, s)[0].start()

    def columns(width):
        return lax.broadcasted_iota(jnp.int32, (extent, width), 1)

    def load(j, s, p, off, turn):
        value = pltpu.roll(jobs[j][1][s, p], (tall - off) % tall, 0)[:extent]
        return pltpu.roll(value, turn, 1)

    def body(s, carry):
        one, off = fetch(0, s)
        one.wait()
        short = slack - left_pos[1, s]
        at = columns(RIM) - short
        good = (at >= 0) & (at + 1 <= left_pos[1, slots])
        for p in range(2):
            out_left[s, p] = jnp.where(good, load(0, s, p, off, short % RIM), 0.0)
        flush(0, s).start()
        one, off = fetch(1, s)
        one.wait()
        col = right_pos[1, s]
        at = columns(RIM) + col
        good = (at < RIM) & (RIM - at <= right_pos[0, slots])
        for p in range(2):
            out_right[s, p] = jnp.where(good, load(1, s, p, off, (cols - col) % RIM), 0.0)
        flush(1, s).start()
        one, off = fetch(2, s)
        one.wait()
        col = own_pos[1, s]
        at = columns(extent) + col
        middle = (at >= RIM) & (at < RIM + cols)
        left_ok = (t > 0) & (at < RIM) & (RIM - at <= own_pos[0, slots])
        right_ok = (t < end) & (at >= RIM + cols) & (at - RIM - cols + 1 <= own_pos[1, slots])
        rim = left_ok | right_ok
        for p in range(2):
            value = load(2, s, p, off, (cols + RIM - col) % cols)
            out_own[s, p] = jnp.where(middle, value, jnp.where(rim, 0.0, 1.0 - p))
        flush(2, s).start()
        return carry

    lax.fori_loop(0, slots, body, 0)
    for s in range(slots):
        for j in range(3):
            flush(j, s).wait()


def gather_kernel(left_pos, right_pos, own_pos, contrib, from_left,
                  from_right, adjoint, grad, entry, acc, buf_own, buf_left, buf_right, buf_entry,
                  sem_in, sem_entry, sem_grad):
    slots, _, extent, _ = buf_own.shape
    rows, cols = acc.shape[1:]
    tall = extent + PAD
    slack = cols + 2 * RIM - extent
    jobs = ((contrib, buf_own), (from_left, buf_left), (from_right, buf_right))

    def fetch(j, s):
        return pltpu.make_async_copy(jobs[j][0].at[s], jobs[j][1].at[s], sem_in.at[j, s])

    for s in range(slots):
        for j in range(3):
            fetch(j, s).start()
    entry_in = pltpu.make_async_copy(adjoint, buf_entry, sem_entry.at[0])
    entry_out = pltpu.make_async_copy(buf_entry, entry, sem_entry.at[1])
    entry_in.start()
    acc[...] = jnp.zeros(acc.shape, acc.dtype)

    def columns(width):
        return lax.broadcasted_iota(jnp.int32, (extent, width), 1)

    def add(source, s, p, row, good, turn, start, width):
        base, off = aligned(row, rows - tall)
        value = jnp.where(good, pltpu.roll(source[s, p], turn, 1), 0.0)
        value = jnp.concatenate([value, jnp.zeros((PAD, width), jnp.float32)], axis=0)
        acc[p, pl.ds(base, tall), pl.ds(start, width)] += pltpu.roll(value, off, 0)

    def plane(p):
        def body(s, carry):
            if p == 0:
                for j in range(3):
                    fetch(j, s).wait()
            col = own_pos[1, s]
            at = columns(cols) + RIM - col
            good = (at >= 0) & (at < extent)
            add(buf_own, s, p, own_pos[0, s], good, (col + cols - RIM) % cols, 0, cols)
            short = slack - left_pos[1, s]
            at = columns(RIM)
            good = (at + short < RIM) & (at + 1 <= left_pos[1, slots])
            add(buf_left, s, p, left_pos[0, s], good, (cols - short) % RIM, 0, RIM)
            col = right_pos[1, s]
            good = (at >= col) & (RIM - at <= right_pos[0, slots])
            add(buf_right, s, p, right_pos[0, s], good, col % RIM, cols - RIM, RIM)
            return carry

        lax.fori_loop(0, slots, body, 0)

    def flush(p):
        return pltpu.make_async_copy(acc.at[p], grad.at[p], sem_grad.at[p])

    plane(0)
    flush(0).start()
    entry_in.wait()
    entry_out.start()
    plane(1)
    flush(1).start()
    entry_out.wait()
    flush(0).wait()
    flush(1).wait()


ENTER, BEYOND, WHOLE, BACK, OFFER, RELAY = range(1, 7)


def schedule(g, last, slots):
    mid, alone = last - 1, slots - 1
    relays = [(0, RELAY, m) for m in range(g + 1, last + 1)]
    plan = [(0, OFFER, g)] * (0 < g < last)
    if g >= mid:
        return plan + relays + [(s, WHOLE, g) for s in range(slots)]
    lag = 2 * (mid - g) + (g == 0)
    done = 0
    for k in range(slots):
        plan += [(k, ENTER, g)]
        if g > 0 and relays:
            plan += [relays.pop(0)]
        if k >= lag:
            plan += [(done, BACK, g)]
            done += 1
    while done < alone - 2:
        plan += [(done, BACK, g)]
        done += 1
    plan += relays + [(alone, BEYOND, g)]
    while done < alone:
        plan += [(done, BACK, g)]
        done += 1
    return plan


def pipeline_kernel(sections, tiles, counts, own, to_left, to_right, hbm_probe, hbm_phase, hbm_measured,
                    ef_hi, ef_lo, ei_hi, ei_lo, of_hi, of_lo, oi_hi, oi_lo, sort, unsort,
                    adjoint_out, contrib_out, from_left, from_right,
                    probe, phase, measured,
                    windows, left_rim, right_rim, arrived, leaving, backed, adjoint, contrib,
                    lefts, rights, turn, talls, wides, spectrum,
                    sem_in, sem_own, sem_out, send_f, recv_f, send_b, recv_b, send_far, recv_far,
                    send_rim, recv_rim, send_got, recv_got, token):
    g = lax.axis_index("cuts")
    t = lax.axis_index("tile")
    last = sections - 1
    mid = last - 1
    end = tiles - 1
    slots, _, extent, _ = windows.shape
    h = extent // 2
    partner = t + 1 - 2 * (t % 2)
    alone = slots - 1

    loads = [
        pltpu.make_async_copy(src, dst, sem_in.at[i])
        for i, (src, dst) in enumerate(
            ((hbm_phase, phase), (hbm_probe, probe), (hbm_measured, measured)))
    ]

    def own_part(s):
        return pltpu.make_async_copy(own.at[s], windows.at[s], sem_own.at[s])

    barrier = pltpu.get_barrier_semaphore()

    @pl.when(g > 0)
    def _():
        pl.semaphore_signal(barrier, inc=1, device_id={"cuts": g - 1}, device_id_type=MESH)

    @pl.when(g < last)
    def _():
        pl.semaphore_signal(barrier, inc=1, device_id={"cuts": g + 1}, device_id_type=MESH)

    @pl.when(t > 0)
    def _():
        pl.semaphore_signal(barrier, inc=1, device_id={"tile": t - 1}, device_id_type=MESH)

    @pl.when(t < end)
    def _():
        pl.semaphore_signal(barrier, inc=1, device_id={"tile": t + 1}, device_id_type=MESH)

    def exact(x, y):
        return jnp.dot(x, y, preferred_element_type=jnp.float32)

    def each(action):
        def body(s, carry):
            action(s)
            return carry

        lax.fori_loop(0, slots, body, 0)

    for load in loads:
        load.start()
    each(lambda s: own_part(s).start())

    def turn_of(i):
        return (i + alone * ((g + last - 1) // last)) % slots

    forms = ((ef_hi, ef_lo, ei_hi, ei_lo), (of_hi, of_lo, oi_hi, oi_lo))
    for parity in range(2):
        fh, fl, ih, il = forms[parity]
        for inverse, (lh, ll, rh, rl) in enumerate(((fh, fl, ih, il), (ih, il, fh, fl))):
            at = 2 * inverse + parity
            lefts[at, :, :extent] = lh[...]
            lefts[at, :, extent : 2 * extent] = lh[...]
            lefts[at, :, 2 * extent :] = ll[...]
            rights[at, :extent] = rh[...]
            rights[at, extent : 2 * extent] = rh[...]
            rights[at, 2 * extent :] = rl[...]

    peers = (g + last - 1) // last + 1 - g // last + (t + end - 1) // end + 1 - t // end
    pl.semaphore_wait(barrier, peers)

    def rim_copy(side, s):
        src, dst = ((to_left, right_rim), (to_right, left_rim))[side]
        return pltpu.make_async_remote_copy(
            src_ref=src.at[s], dst_ref=dst.at[s], send_sem=send_rim.at[side, s],
            recv_sem=recv_rim.at[side, s], device_id={"tile": t + (-1, 1)[side]},
            device_id_type=MESH)

    def got_copy(side, s):
        start, dst = ((0, from_right), (extent - RIM, from_left))[side]
        return pltpu.make_async_remote_copy(
            src_ref=contrib.at[s, :, :, pl.ds(start, RIM)], dst_ref=dst.at[s],
            send_sem=send_got.at[side, s], recv_sem=recv_got.at[side, s],
            device_id={"tile": t + (-1, 1)[side]}, device_id_type=MESH)

    yielding = (t % 2 == 0) & (t > 0)

    def rims_start(side, s, ok):
        @pl.when(ok)
        def _():
            rim_copy(side, s).start()

    def rims_one(i):
        s = turn_of(i)
        rims_start(0, s, (t > 0) & jnp.logical_not(yielding))
        rims_start(1, s, t < end)

    each(rims_one)

    @pl.when(yielding)
    def _():
        rim_copy(0, turn_of(0)).wait_recv()

    each(lambda i: rims_start(0, turn_of(i), yielding))

    @pl.when(t == 0)
    def _():
        left_rim[...] = jnp.zeros(left_rim.shape, left_rim.dtype)

    @pl.when(t == end)
    def _():
        right_rim[...] = jnp.zeros(right_rim.shape, right_rim.dtype)

    loads[0].wait()
    rest = phase[...]
    total = jnp.zeros((extent, extent), jnp.float32)
    for _ in range(3):
        part = rest.astype(jnp.bfloat16)
        rest = rest - part.astype(jnp.float32)
        total += exact(exact(sort[...], part).astype(jnp.bfloat16), unsort[...])
    turn[0] = jnp.cos(total)
    sine = jnp.sin(total)
    turn[1] = sine
    turn[2] = -sine
    loads[1].wait()
    loads[2].wait()

    def split(value):
        hi = value.astype(jnp.bfloat16)
        lo = (value - hi.astype(jnp.float32)).astype(jnp.bfloat16)
        return (hi, lo, hi)

    def put_tall(parity, p, value):
        for at, part in enumerate(split(value)):
            talls[parity, pl.ds(at * extent + p * h, h), :] = part

    def put_wide(parity, rows, p, value):
        n = value.shape[0]
        for at, part in enumerate(split(value)):
            wides[parity, pl.ds(rows, n), pl.ds(at * extent + p * h, h)] = part

    def left(at):
        return exact(lefts[at], talls[at % 2])

    def right(at):
        return exact(wides[at % 2], rights[at])

    def halves(load):
        upper, lower = load(slice(0, h)), load(slice(h, extent))
        for p in range(2):
            put_tall(0, p, upper[p] + lower[p])
            put_tall(1, p, upper[p] - lower[p])

    def plain(ref, *at):
        def load(rows):
            return [ref[(*at, p, rows)] for p in range(2)]

        return load

    def through(w, w_at, x, x_at, sign):
        def load(rows):
            wr, wi = w[w_at, 0, rows], w[w_at, 1, rows]
            xr, xi = x[(*x_at, 0, rows)], x[(*x_at, 1, rows)]
            if sign > 0:
                return [wr * xr - wi * xi, wr * xi + wi * xr]
            return [wr * xr + wi * xi, wr * xi - wi * xr]

        return load

    def turned(sine):
        def middle(parity, xr, xi):
            cols = slice(parity * h, (parity + 1) * h)
            kr, ki = turn[0, :, cols], turn[sine, :, cols]
            return kr * xr - ki * xi, kr * xi + ki * xr

        return middle

    def transform(load, middle):
        halves(load)
        for block in range(2):
            half = left(block)
            for p in range(2):
                value = half[p * h : (p + 1) * h]
                put_wide(0, block * h, p, value[:, :h] + value[:, h:])
                put_wide(1, block * h, p, value[:, :h] - value[:, h:])
        for parity in range(2):
            value = right(parity)
            for p, part in enumerate(middle(parity, value[:, :h], value[:, h:])):
                put_wide(parity, 0, p, part)
        u, v = right(2), right(3)
        for p in range(2):
            up, vp = u[:, p * h : (p + 1) * h], v[:, p * h : (p + 1) * h]
            plus, minus = up + vp, up - vp
            for parity in range(2):
                rows = slice(parity * h, (parity + 1) * h)
                put_tall(parity, p, jnp.concatenate([plus[rows], minus[rows]], axis=1))
        u, v = left(2), left(3)
        for p in range(2):
            up, vp = u[p * h : (p + 1) * h], v[p * h : (p + 1) * h]
            spectrum[p, :h] = up + vp
            spectrum[p, h:] = up - vp

    def send_forward(s, part):
        return pltpu.make_async_remote_copy(
            src_ref=leaving.at[s, part], dst_ref=arrived.at[s, part], send_sem=send_f.at[s, part],
            recv_sem=recv_f.at[s, part], device_id={"cuts": g + 1}, device_id_type=MESH)

    def send_backward(s):
        return pltpu.make_async_remote_copy(
            src_ref=adjoint.at[s], dst_ref=backed.at[s], send_sem=send_b.at[s],
            recv_sem=recv_b.at[s], device_id={"cuts": g - 1}, device_id_type=MESH)

    def send_window(s):
        return pltpu.make_async_remote_copy(
            src_ref=windows.at[s], dst_ref=backed.at[s], send_sem=send_b.at[s],
            recv_sem=recv_b.at[s], device_id={"cuts": g - 1}, device_id_type=MESH)

    def far_at(m):
        return slots + m - 1

    def send_own_far():
        return pltpu.make_async_remote_copy(
            src_ref=windows.at[alone], dst_ref=backed.at[far_at(g)], send_sem=send_far.at[g],
            recv_sem=recv_far.at[g], device_id={"cuts": g - 1}, device_id_type=MESH)

    def send_far_on(m):
        return pltpu.make_async_remote_copy(
            src_ref=backed.at[far_at(m)], dst_ref=backed.at[far_at(m)], send_sem=send_far.at[m],
            recv_sem=recv_far.at[m], device_id={"cuts": g - 1}, device_id_type=MESH)

    def compose(s):
        own_part(s).wait()

        @pl.when((t < end) & jnp.logical_not(yielding & (s == turn_of(0))))
        def _():
            rim_copy(0, s).wait_recv()

        @pl.when(t > 0)
        def _():
            rim_copy(1, s).wait_recv()

        for p in range(2):
            windows[s, p, :, :RIM] += left_rim[s, p]
            windows[s, p, :, extent - RIM :] += right_rim[s, p]

    def put_out(j, s):
        src, dst = ((adjoint, adjoint_out), (contrib, contrib_out))[j]
        return pltpu.make_async_copy(src.at[s], dst.at[s], sem_out.at[j, s])

    @pl.when(g == last)
    def _():
        def body(i):
            s = turn_of(i)
            compose(s)

            @pl.when(s == alone)
            def _():
                send_own_far().start()

            @pl.when(s < alone)
            def _():
                send_window(s).start()

        each(body)

    def enter(s):
        @pl.when(g == 0)
        def _():
            arrived[s] = probe[...] * jnp.clip(counts[0] - s, 0, 1).astype(jnp.float32)

        @pl.when(g > 0)
        def _():
            send_forward(s, 0).wait_recv()
            send_forward(s, 1).wait_recv()

        @pl.when((g < last) & ((g == 0) | (s < alone)))
        def _():
            compose(s)

        transform(through(windows, s, arrived, (s,), 1), turned(1))

        @pl.when(g < last)
        def _():
            leaving[s] = spectrum[...]

            @pl.when((g == 0) & ((s > 0) | (t % 2 == 1)))
            def _():
                pl.semaphore_wait(token, 1)

            send_forward(s, 0).start()
            send_forward(s, 1).start()

            @pl.when(g == 0)
            def _():
                send_forward(s, 0).wait_send()

                @pl.when((s < slots - 1) | (t % 2 == 0))
                def _():
                    pl.semaphore_signal(token, inc=1, device_id={"tile": partner}, device_id_type=MESH)

    def beyond(s):
        later = last - g

        @pl.when((g == mid) & (s < alone))
        def _():
            send_window(s).wait_recv()

        @pl.when(g < mid)
        def _():
            spectrum[...] = leaving[s]

        def onward(i, carry):
            spot = jnp.where(s == alone, far_at(g + 1 + i), s)
            transform(through(backed, spot, spectrum, (), 1), turned(1))
            return carry

        lax.fori_loop(0, later, onward, 0)
        seen = exact(sort[...], measured[s]).astype(jnp.bfloat16)
        seen = exact(seen, unsort[...])

        def detected(parity, xr, xi):
            residual = xr * xr + xi * xi - seen[:, parity * h : (parity + 1) * h]
            return xr * residual, xi * residual

        transform(plain(spectrum), detected)
        transform(plain(spectrum), turned(2))

        def homeward(i, carry):
            spot = jnp.where(s == alone, far_at(last - i), s)
            transform(through(backed, spot, spectrum, (), -1), turned(2))
            return carry

        lax.fori_loop(0, later, homeward, 0)

    def back(s):
        send_backward(s).wait_recv()
        transform(plain(backed, s), turned(2))

    def finish_slot(s):
        tr, ti = spectrum[0], spectrum[1]
        wr, wi = windows[s, 0], windows[s, 1]
        adjoint[s, 0] = wr * tr + wi * ti
        adjoint[s, 1] = wr * ti - wi * tr

        @pl.when((g > 0) & (g < last) & (s < alone))
        def _():
            send_backward(s).start()

        xr, xi = arrived[s, 0], arrived[s, 1]
        contrib[s, 0] = xr * tr + xi * ti
        contrib[s, 1] = xr * ti - xi * tr

        @pl.when(t > 0)
        def _():
            got_copy(0, s).start()

        @pl.when(t < end)
        def _():
            got_copy(1, s).start()

        put_out(0, s).start()
        put_out(1, s).start()

    plans = [schedule(here, last, slots) for here in range(sections)]
    width = max(len(plan) for plan in plans)

    def step(e, carry):
        code = jnp.int32(0)
        for here, plan in enumerate(plans):
            for at, (s, act, m) in enumerate(plan):
                code = jnp.where((g == here) & (e == at), (s * 8 + act) * (sections + 1) + m + 1, code)
        m, rest = code % (sections + 1) - 1, code // (sections + 1)
        act, s = rest % 8, rest // 8

        @pl.when((act == ENTER) | (act == WHOLE))
        def _():
            enter(s)

        @pl.when((act == BEYOND) | (act == WHOLE))
        def _():
            beyond(s)

        @pl.when(act == BACK)
        def _():
            back(s)

        @pl.when((act == BEYOND) | (act == WHOLE) | (act == BACK))
        def _():
            finish_slot(s)

        @pl.when(act == OFFER)
        def _():
            compose(alone)
            send_own_far().start()

        @pl.when(act == RELAY)
        def _():
            send_far_on(m).wait_recv()

            @pl.when(g > 0)
            def _():
                send_far_on(m).start()

        return carry

    lax.fori_loop(0, width, step, 0)

    def all_but_lone(action):
        def body(s, carry):
            action(s)
            return carry

        lax.fori_loop(0, alone, body, 0)

    @pl.when(g < last)
    def _():
        each(lambda s: send_forward(s, 1).wait_send())

    @pl.when((g > 0) & (g < last))
    def _():
        each(lambda s: send_forward(s, 0).wait_send())
        all_but_lone(lambda s: send_backward(s).wait_send())

    @pl.when(g == last)
    def _():
        all_but_lone(lambda s: send_window(s).wait_send())

    @pl.when(g > 0)
    def _():
        send_own_far().wait_send()

    for m in range(2, sections):
        @pl.when((g > 0) & (g < m))
        def _():
            send_far_on(m).wait_send()

    @pl.when(t < end)
    def _():
        each(lambda s: got_copy(0, s).wait_recv())

    @pl.when(t > 0)
    def _():
        each(lambda s: got_copy(1, s).wait_recv())

    def finish(side):
        def body(s):
            rim_copy(side, s).wait_send()
            got_copy(side, s).wait_send()

        each(body)

    @pl.when(t > 0)
    def _():
        finish(0)

    @pl.when(t < end)
    def _():
        finish(1)

    each(lambda s: put_out(0, s).wait())
    each(lambda s: put_out(1, s).wait())


def on_device(probe_wave, transmission, kernel_phase, measured, counts, positions, widths):
    f32 = jnp.float32
    bf16 = jnp.bfloat16
    rows, cols = transmission.shape[2:]
    extent = probe_wave.shape[-1]
    slots = positions.shape[1]
    sections = lax.axis_size("cuts")
    tiles = lax.axis_size("tile")
    assert extent == cols and extent >= 2 * RIM and tiles % 2 == 0 and sections >= 2
    sds = jax.ShapeDtypeStruct
    wave = sds((slots, 2, extent, extent), f32)
    rim = sds((slots, 2, extent, RIM), f32)
    waves = pltpu.VMEM(wave.shape, f32)
    rims = pltpu.VMEM(rim.shape, f32)
    hbm = pl.BlockSpec(memory_space=pl.ANY)
    dma = pltpu.SemaphoreType.DMA
    tall = extent + PAD
    marks = sds((2, slots + 1), jnp.int32)
    left_pos, right_pos, own_pos = pl.pallas_call(
        functools.partial(exchange_kernel, tiles),
        out_shape=(marks,) * 3,
        in_specs=[smem()] * 2,
        out_specs=(smem(),) * 3,
        scratch_shapes=[
            pltpu.SMEM((2, 2, slots), jnp.int32),
            pltpu.SMEM((2, 1, 2), jnp.int32),
            dma((2, 2)), dma((2, 2)),
        ],
        compiler_params=params(EXTRACT_VMEM, collective_id=1, has_side_effects=True),
    )(jnp.swapaxes(positions[0], 0, 1), widths)
    own, to_left, to_right = pl.pallas_call(
        extract_kernel,
        out_shape=(wave, rim, rim),
        in_specs=[smem()] * 3 + [hbm],
        out_specs=(hbm,) * 3,
        scratch_shapes=[
            pltpu.VMEM((slots, 2, tall, RIM), f32),
            pltpu.VMEM((slots, 2, tall, RIM), f32),
            pltpu.VMEM((slots, 2, tall, cols), f32),
            rims, rims, waves,
            dma((3, slots)), dma((3, slots)),
        ],
        compiler_params=params(EXTRACT_VMEM),
    )(left_pos, right_pos, own_pos, transmission[0])
    adjoint, contrib, from_left, from_right = pl.pallas_call(
        functools.partial(pipeline_kernel, sections, tiles),
        out_shape=(wave, wave, rim, rim),
        in_specs=[smem()] + [hbm] * 6 + [vmem()] * 10,
        out_specs=(hbm,) * 4,
        scratch_shapes=[
            pltpu.VMEM((2, extent, extent), f32),
            pltpu.VMEM((extent, extent), f32),
            pltpu.VMEM((slots, extent, extent), bf16),
            waves, rims, rims,
            waves, waves,
            pltpu.VMEM((slots + sections - 1, 2, extent, extent), f32),
            waves, waves,
            pltpu.VMEM((4, extent, 3 * extent), bf16),
            pltpu.VMEM((4, 3 * extent, extent), bf16),
            pltpu.VMEM((3, extent, extent), f32),
            pltpu.VMEM((2, 3 * extent, extent), bf16),
            pltpu.VMEM((2, extent, 3 * extent), bf16),
            pltpu.VMEM((2, extent, extent), f32),
            dma((3,)),
            dma((slots,)),
            dma((2, slots)),
            dma((slots, 2)), dma((slots, 2)),
            dma((slots,)), dma((slots,)),
            dma((sections,)), dma((sections,)),
            dma((2, slots)), dma((2, slots)),
            dma((2, slots)), dma((2, slots)),
            pltpu.SemaphoreType.REGULAR,
        ],
        compiler_params=params(PIPELINE_VMEM, collective_id=0, has_side_effects=True),
    )(counts, own, to_left, to_right, probe_wave, kernel_phase, measured[0], *make_tables(extent))
    grad, entry = pl.pallas_call(
        gather_kernel,
        out_shape=(sds((2, rows, cols), f32), wave),
        in_specs=[smem()] * 3 + [hbm] * 4,
        out_specs=(hbm, hbm),
        scratch_shapes=[
            pltpu.VMEM((2, rows, cols), f32), waves, rims, rims, waves,
            dma((3, slots)), dma((2,)), dma((2,)),
        ],
        compiler_params=params(GATHER_VMEM),
    )(left_pos, right_pos, own_pos, contrib, from_left, from_right, adjoint)
    return (entry[None, None], grad[None])


def solution(mesh):
    return jax.shard_map(
        on_device,
        mesh=mesh,
        in_specs=(
            P(),
            P("cuts", None, None, "tile"),
            P(),
            P("tile", None, None, None),
            P("tile"),
            P("tile", None, None),
            P("tile", None),
        ),
        out_specs=(P("cuts", "tile", None, None, None, None), P("cuts", None, None, "tile")),
        check_vma=False,
    )
```
